32 devices in a mesh: group: 4 (over z), patch: 8 (over y, x, core).
Axes of the slice: x: 2, y: 2, z: 4, core: 2. Of those that a mesh axis runs over, the one named last changes fastest.
Arguments:
- node_latent: bfloat16 [10240, 512], P(('group', 'patch')), may hold values from -6 to 6
- fine_latent: bfloat16 [65536, 512], P(('group', 'patch')), may hold values from -6 to 6
- coarse_latent: bfloat16 [16384, 512], P(('group', 'patch')), may hold values from -6 to 6
- fine_sender: int32 [65536], P(('group', 'patch')), may hold values from 0 to 447
- fine_receiver: int32 [65536], P(('group', 'patch')), may hold values from 0 to 319
- coarse_owner: int32 [16384, 1], P(('group', 'patch')), may hold values from 0 to 31; in each aligned block of 512 rows (0 to 511, 512 to 1023, ...) at most 32 rows name the same one
- coarse_row: int32 [16384], P(('group', 'patch')), may hold values from 0 to 15
- coarse_receiver: int32 [16384], P(('group', 'patch')), may hold values from 0 to 15
- edge_first: bfloat16 [2, 1536, 512], replicated, may hold values from -0.15625 to 0.15625
- edge_bias: float32 [2, 512], replicated, may hold values from -3 to 3
- edge_second: bfloat16 [2, 512, 512], replicated, may hold values from -0.25 to 0.25
- edge_gain: float32 [2, 512], replicated, may hold values from 0.25 to 1.75
- node_first: bfloat16 [2, 1024, 512], replicated, may hold values from -0.1875 to 0.1875
- node_bias: float32 [2, 512], replicated, may hold values from -3 to 3
- node_second: bfloat16 [2, 512, 512], replicated, may hold values from -0.25 to 0.25
- node_gain: float32 [2, 512], replicated, may hold values from 0.25 to 1.75
Outputs:
- node_out: bfloat16 [10240, 512], P(('group', 'patch'))
- fine_out: bfloat16 [65536, 512], P(('group', 'patch'))
- coarse_out: bfloat16 [16384, 512], P(('group', 'patch'))
The draws below stay inside these ranges and needn't reach their ends.
Inputs may be any that keep to these rules, and one draw needn't show every extreme that they name: `fine_sender`: A fine edge's sender indexes the receiving device's patch extended by 64 nodes on each side: values below 64 are the last 64 nodes of the previous patch of the same group, values from 384 on the first 64 nodes of the next patch; patches of a group close into a loop. `coarse_owner`: among the 512 coarse edges of one device, at most 32 have their sender on any one device.
All inputs are finite; a program needn't handle non-finite values.
Results may differ from the reference program's by a relative error of at most 0.0095.
Values may be sent and summed in bfloat16 or wider, within the bound.
No kernel may reach another device: no remote copies, remote signals or barrier semaphores. Data moves between devices by JAX's collectives and lax.ppermute only.
A program may use at most 128 MiB of HBM per device.

```python
import math
import jax
import jax.numpy as jnp
import numpy as np
from jax import lax

D = 512
NODE_DEV = 320
FINE_DEV = 2048
CE_DEV = 512
HALO = 64
COARSE = 16
LAYERS = 2
CAP = 32
NODES = 10240
FINE_EDGES = 65536
COARSE_EDGES = 16384
N_GROUP = 4
N_PATCH = 8
DEVICES = 32


def touch_ends(entries, stream_key, least, largest):
    place = [jax.random.randint(jax.random.fold_in(stream_key, axis), (), 0, length) for axis, length in enumerate(entries.shape)]
    main_axis = entries.shape.index(max(entries.shape))
    beside = place[:main_axis] + [(place[main_axis] + 1) % entries.shape[main_axis]] + place[main_axis + 1:]
    return entries.at[tuple(place)].set(least).at[tuple(beside)].set(largest)


def block_levels(key, dims, pieces, low, high):
    def one(dim, parts):
        steps = jax.random.uniform(jax.random.fold_in(jax.random.fold_in(key, 6), dim), (parts,), jnp.float32, low / len(pieces), high / len(pieces))
        return jnp.repeat(jnp.exp(steps), dims[dim] // parts).reshape((-1,) + (1,) * (len(dims) - dim - 1))

    gain = one(*pieces[0])
    for cut in pieces[1:]:
        gain = gain * one(*cut)
    return gain


def deal_out(stream_key, own, number, rows, count, top, most, slope):
    sequence = jax.random.permutation(stream_key, count)
    heavy_load, usual = portions_of(count, rows * top, most, slope, True), portions_of(count, rows * top, most, slope, False)
    places = jnp.arange(count)

    def named(tallies, offset_by):
        used = int((tallies > 0).sum())
        fixed = max(1, used // 4)
        passed = fixed + (places - fixed + offset_by * (used - fixed)) % max(1, count - fixed)
        return jnp.zeros((count,), jnp.int32).at[sequence[jnp.where(places < fixed, places, passed)]].set(jnp.asarray(tallies, jnp.int32))

    tallies = jnp.where(number % 4 == 0, named(heavy_load, number // 4), named(usual, number - number // 4 - 1))
    mixed = jax.random.permutation(jax.random.fold_in(own, 3), count)
    giver, taker = mixed[0:count // 2 * 2:2], mixed[1:count // 2 * 2:2]
    margin = jnp.minimum(tallies[giver] - 1, most - tallies[taker]) // 2
    margin = jnp.where((giver == sequence[0]) | (taker == sequence[0]) | (tallies[taker] == 0), 0, jnp.maximum(margin, 0))
    passed = jax.random.randint(jax.random.fold_in(own, 4), (count // 2,), 0, 1 << 20) % (margin + 1)
    tallies = tallies.at[giver].add(-passed).at[taker].add(passed)
    labels = jnp.searchsorted(jnp.cumsum(tallies), jnp.arange(rows * top), side="right").astype(jnp.int32)
    grid = labels.reshape(top, rows).T
    grid = grid[jax.random.permutation(jax.random.fold_in(own, 1), rows)]
    offset_by = jax.random.randint(jax.random.fold_in(own, 2), (rows, 1), 0, top)
    return jnp.take_along_axis(grid, (jnp.arange(top)[None, :] + offset_by) % top, axis=1)


def portions_of(count, total, reach, lean, full):
    weights = [(1 << 20) // math.isqrt(grade ** lean) + 1 for grade in range(1, count + 1)]
    largest = reach if full else min(reach, max(-(-total // count), total * weights[0] // sum(weights)))
    least = 1 if total - largest >= count - 1 else 0
    holding, spare = [largest] + [least] * (count - 1), total - largest - least * (count - 1)
    while spare > 0:
        movable = [i for i in range(1, count) if holding[i] < largest] or [i for i in range(1, count) if holding[i] < reach]
        pool, left = sum([weights[i] for i in movable]), spare
        for i in movable:
            extra = min(reach - holding[i], max(1, left * weights[i] // pool), spare)
            holding[i] = holding[i] + extra
            spare = spare - extra
    return np.array(holding)


def normal_values(stream_key, extent, width, bound, split=(), held_as=jnp.bfloat16):
    array = jax.random.normal(stream_key, extent, jnp.float32) * width
    if len(split) > 0:
        array = block_levels(stream_key, extent, split, -0.22, 0.18) * array
    return jnp.clip(array, min=-bound, max=bound).astype(held_as)


def setup_inputs(seed: int = 0) -> dict:
    seeds = jax.random.split(jax.random.key(seed), 17)
    node_latent = normal_values(seeds[0], (NODES, D), 1.0, 6.0, ((0, 32),))
    fine_latent = normal_values(seeds[1], (FINE_EDGES, D), 1.0, 6.0, ((0, 32),))
    coarse_latent = normal_values(seeds[2], (COARSE_EDGES, D), 1.0, 6.0, ((0, 32),))
    fine_sender = touch_ends(jax.random.randint(seeds[3], (FINE_EDGES,), 0, NODE_DEV + 2 * HALO), jax.random.fold_in(seeds[3], 1), 0, (NODE_DEV + 2 * HALO) - 1).astype(jnp.int32)
    fine_receiver = touch_ends(jax.random.randint(seeds[4], (FINE_EDGES,), 0, NODE_DEV), jax.random.fold_in(seeds[4], 1), 0, NODE_DEV - 1).astype(jnp.int32)
    coarse_owner_keys = jax.random.split(jax.random.fold_in(seeds[5], 1), COARSE_EDGES // CE_DEV)
    coarse_owner_turns = jax.random.permutation(jax.random.fold_in(seeds[5], 3), COARSE_EDGES // CE_DEV)
    coarse_owner = jax.vmap(lambda own, number: deal_out(jax.random.fold_in(seeds[5], 2), own, number, CE_DEV, DEVICES, 1, CAP, 2))(coarse_owner_keys, coarse_owner_turns).reshape((COARSE_EDGES, 1))
    coarse_row = touch_ends(jax.random.randint(seeds[6], (COARSE_EDGES,), 0, COARSE), jax.random.fold_in(seeds[6], 1), 0, COARSE - 1).astype(jnp.int32)
    coarse_receiver = touch_ends(jax.random.randint(seeds[7], (COARSE_EDGES,), 0, COARSE), jax.random.fold_in(seeds[7], 1), 0, COARSE - 1).astype(jnp.int32)
    edge_first = normal_values(seeds[8], (LAYERS, 3 * D, D), (3 * D) ** -0.5, 0.15625)
    edge_bias = normal_values(seeds[9], (LAYERS, D), 0.5, 3.0, (), jnp.float32)
    edge_second = normal_values(seeds[10], (LAYERS, D, D), D ** -0.5, 0.25)
    edge_gain = jnp.clip(1.0 + 0.15 * jax.random.normal(seeds[11], (LAYERS, D), jnp.float32), 0.25, 1.75)
    node_first = normal_values(seeds[12], (LAYERS, 2 * D, D), (2 * D) ** -0.5, 0.1875)
    node_bias = normal_values(seeds[13], (LAYERS, D), 0.5, 3.0, (), jnp.float32)
    node_second = normal_values(seeds[14], (LAYERS, D, D), D ** -0.5, 0.25)
    node_gain = jnp.clip(1.0 + 0.15 * jax.random.normal(seeds[15], (LAYERS, D), jnp.float32), 0.25, 1.75)
    return {"node_latent": node_latent, "fine_latent": fine_latent, "coarse_latent": coarse_latent, "fine_sender": fine_sender, "fine_receiver": fine_receiver, "coarse_owner": coarse_owner, "coarse_row": coarse_row, "coarse_receiver": coarse_receiver, "edge_first": edge_first, "edge_bias": edge_bias, "edge_second": edge_second, "edge_gain": edge_gain, "node_first": node_first, "node_bias": node_bias, "node_second": node_second, "node_gain": node_gain}


EPSILON = 1e-05

def norm_rows(values, gain_row):
    centre = lax.optimization_barrier(jnp.mean(values, axis=-1, keepdims=True))
    centred = values - centre
    variance = lax.optimization_barrier(jnp.mean(centred * centred, axis=-1, keepdims=True))
    return centred * lax.rsqrt(variance + EPSILON) * gain_row

def edge_block(latent, from_sender, from_receiver, weight_edge, bias_row, weight_second, gain_row):
    pre = jnp.dot(latent, weight_edge, preferred_element_type=jnp.float32) + from_sender + from_receiver + bias_row
    hidden = jax.nn.silu(pre).astype(jnp.bfloat16)
    output = jnp.dot(hidden, weight_second, preferred_element_type=jnp.float32)
    message = norm_rows(output, gain_row)
    updated = (latent.astype(jnp.float32) + message).astype(jnp.bfloat16)
    return (updated, message.astype(jnp.bfloat16))

def reference(node_latent, fine_latent, coarse_latent, fine_sender, fine_receiver, coarse_owner, coarse_row, coarse_receiver, edge_first, edge_bias, edge_second, edge_gain, node_first, node_bias, node_second, node_gain):
    devices = N_GROUP * N_PATCH
    fine_device = jnp.arange(FINE_DEV * devices, dtype=jnp.int32) // FINE_DEV
    group_index = fine_device // N_PATCH
    patch_index = fine_device % N_PATCH
    within = (patch_index * NODE_DEV + fine_sender - HALO) % (N_PATCH * NODE_DEV)
    fine_global = (group_index * (N_PATCH * NODE_DEV) + within).astype(jnp.int32)
    fine_target = (fine_device * NODE_DEV + fine_receiver).astype(jnp.int32)
    coarse_device = jnp.arange(CE_DEV * devices, dtype=jnp.int32) // CE_DEV
    coarse_global = (coarse_owner[:, 0] * NODE_DEV + coarse_row).astype(jnp.int32)
    coarse_target = (coarse_device * NODE_DEV + coarse_receiver).astype(jnp.int32)
    targets = jnp.concatenate([fine_target, coarse_target]).astype(jnp.int32)
    latent = node_latent
    fine_state = fine_latent
    coarse_state = coarse_latent
    for layer_index in range(LAYERS):
        first = edge_first[layer_index]
        weight_edge = first[:D]
        sender_proj = jnp.dot(latent, first[D:2 * D], preferred_element_type=jnp.float32)
        receiver_proj = jnp.dot(latent, first[2 * D:], preferred_element_type=jnp.float32)
        bias_row = edge_bias[layer_index]
        weight_second = edge_second[layer_index]
        gain_row = edge_gain[layer_index]

        def run_block(packed):
            block_latent, block_sender, block_receiver = packed
            return edge_block(block_latent, jnp.take(sender_proj, block_sender, axis=0), jnp.take(receiver_proj, block_receiver, axis=0), weight_edge, bias_row, weight_second, gain_row)
        fine_new, fine_message = lax.map(run_block, (fine_state.reshape(devices, FINE_DEV, D), fine_global.reshape(devices, FINE_DEV), fine_target.reshape(devices, FINE_DEV)))
        coarse_new, coarse_message = lax.map(run_block, (coarse_state.reshape(devices, CE_DEV, D), coarse_global.reshape(devices, CE_DEV), coarse_target.reshape(devices, CE_DEV)))
        fine_state = fine_new.reshape(-1, D)
        coarse_state = coarse_new.reshape(-1, D)
        messages = jnp.concatenate([fine_message.reshape(-1, D), coarse_message.reshape(-1, D)]).astype(jnp.float32)
        summed = jax.ops.segment_sum(messages, targets, num_segments=NODE_DEV * devices).astype(jnp.bfloat16)
        node_weights = node_first[layer_index]
        pre = jnp.dot(latent, node_weights[:D], preferred_element_type=jnp.float32) + jnp.dot(summed, node_weights[D:], preferred_element_type=jnp.float32) + node_bias[layer_index]
        hidden = jax.nn.silu(pre).astype(jnp.bfloat16)
        output = jnp.dot(hidden, node_second[layer_index], preferred_element_type=jnp.float32)
        latent = (latent.astype(jnp.float32) + norm_rows(output, node_gain[layer_index])).astype(jnp.bfloat16)
    return (latent, fine_state, coarse_state)
```

```python
import functools

import jax
import jax.numpy as jnp
from jax import lax
from jax.experimental import pallas as pl
from jax.experimental.pallas import tpu as pltpu
from jax.sharding import PartitionSpec as P

HALO = 64
COARSE = 16
EPSILON = 1e-05
GP = ("group", "patch")


def dot(a, b):
    return jnp.dot(a, b, preferred_element_type=jnp.float32)


def half_silu(half):
    return half * jnp.tanh(half) + half


def centred_columns(weight):
    wide = weight.astype(jnp.float32)
    return (wide - jnp.mean(wide, axis=-1, keepdims=True)).astype(jnp.bfloat16)


def scale_rows(centred, gain_row):
    variance = jnp.mean(centred * centred, axis=-1, keepdims=True)
    return centred * lax.rsqrt(variance + EPSILON) * gain_row


def column_of(row):
    return jnp.transpose(jnp.broadcast_to(row, (128, row.shape[1])))


def onehot_lanes(column, count):
    lanes = lax.broadcasted_iota(jnp.int32, column.shape, 1)
    parts = [
        jnp.where(column == lanes + start, 1.0, 0.0).astype(jnp.bfloat16)
        for start in range(0, count, 128)
    ]
    return jnp.concatenate(parts, axis=1)


def onehot_sublanes(row, count):
    places = lax.broadcasted_iota(jnp.int32, (count, row.shape[1]), 0)
    return jnp.where(places == row, 1.0, 0.0).astype(jnp.bfloat16)


def edge_rows(latent, ends, table, weight_edge, weight_second, gain_row):
    half = dot(latent, weight_edge) + dot(ends, table)
    hidden = half_silu(half).astype(jnp.bfloat16)
    message = scale_rows(dot(hidden, weight_second), gain_row)
    updated = (latent.astype(jnp.float32) + message).astype(jnp.bfloat16)
    return updated, message.astype(jnp.bfloat16)


def fine_kernel(
    layer, sub, e_ref, snd_ref, rcv_ref, h_ref, lo_ref, hi_ref, first_ref, bias_ref, second_ref, gain_ref,
    out_ref, agg_ref, table, w_edge, w_second,
):
    width = h_ref.shape[1]
    nodes = h_ref.shape[0]
    senders = nodes + 2 * HALO

    @pl.when(pl.program_id(0) == 0)
    def _():
        w_s = first_ref[0, width : 2 * width, :]
        h = h_ref[...]
        table[0:HALO, :] = (dot(lo_ref[...], w_s) * 0.5).astype(jnp.bfloat16)
        table[HALO : HALO + nodes, :] = (dot(h, w_s) * 0.5).astype(jnp.bfloat16)
        table[HALO + nodes : senders, :] = (dot(hi_ref[...], w_s) * 0.5).astype(jnp.bfloat16)
        received = dot(h, first_ref[0, 2 * width :, :]) + bias_ref[layer : layer + 1, :]
        table[senders:, :] = (received * 0.5).astype(jnp.bfloat16)
        w_edge[...] = (first_ref[0, 0:width, :] * 0.5).astype(jnp.bfloat16)
        w_second[...] = centred_columns(second_ref[0])
        agg_ref[...] = jnp.zeros_like(agg_ref)

    gain_row = gain_ref[layer : layer + 1, :]
    total = agg_ref[...]
    for start in range(0, e_ref.shape[0], sub):
        rows = slice(start, start + sub)
        snd = snd_ref[0, :, rows]
        rcv = rcv_ref[0, :, rows]
        from_sender = column_of(snd)
        from_receiver = column_of(rcv) + senders
        lanes = lax.broadcasted_iota(jnp.int32, from_sender.shape, 1)
        parts = []
        for place in range(0, senders + nodes, 128):
            hit = None
            if place < senders:
                hit = from_sender == lanes + place
            if place + 128 > senders:
                other = from_receiver == lanes + place
                hit = other if hit is None else hit | other
            parts.append(jnp.where(hit, 1.0, 0.0).astype(jnp.bfloat16))
        ends = jnp.concatenate(parts, axis=1)
        updated, message = edge_rows(e_ref[rows, :], ends, table[...], w_edge[...], w_second[...], gain_row)
        out_ref[rows, :] = updated
        total += dot(onehot_sublanes(rcv, nodes), message)
    agg_ref[...] = total


def fine_call(layer, e, snd, rcv, h, lo, hi, first, bias, second, gain, block, sub):
    edges, width = e.shape
    nodes = h.shape[0]
    steps = edges // block
    table_rows = 2 * nodes + 2 * HALO
    whole = lambda i: (0, 0)
    this_layer = lambda i: (layer, 0, 0)
    return pl.pallas_call(
        functools.partial(fine_kernel, layer, sub),
        grid=(steps,),
        in_specs=[
            pl.BlockSpec((block, width), lambda i: (i, 0)),
            pl.BlockSpec((1, 1, block), lambda i: (i, 0, 0)),
            pl.BlockSpec((1, 1, block), lambda i: (i, 0, 0)),
            pl.BlockSpec((nodes, width), whole),
            pl.BlockSpec((HALO, width), whole),
            pl.BlockSpec((HALO, width), whole),
            pl.BlockSpec((1,) + first.shape[1:], this_layer),
            pl.BlockSpec(bias.shape, whole),
            pl.BlockSpec((1,) + second.shape[1:], this_layer),
            pl.BlockSpec(gain.shape, whole),
        ],
        out_specs=[
            pl.BlockSpec((block, width), lambda i: (i, 0)),
            pl.BlockSpec((nodes, width), whole),
        ],
        out_shape=[
            jax.ShapeDtypeStruct((edges, width), jnp.bfloat16),
            jax.ShapeDtypeStruct((nodes, width), jnp.float32),
        ],
        scratch_shapes=[
            pltpu.VMEM((table_rows, width), jnp.bfloat16),
            pltpu.VMEM((width, width), jnp.bfloat16),
            pltpu.VMEM((width, width), jnp.bfloat16),
        ],
        cost_estimate=pl.CostEstimate(
            flops=2 * edges * width * (2 * width + 2 * table_rows), bytes_accessed=8 << 20, transcendentals=0
        ),
        name=f"fine_{layer}",
    )(e, snd.reshape(steps, 1, block), rcv.reshape(steps, 1, block), h, lo, hi, first, bias, second, gain)


def coarse_kernel(
    layer, sub, e_ref, idx_ref, rcv_ref, near_ref, far_ref, h_ref, agg_ref, first_ref, bias_ref, second_ref, gain_ref,
    node_first_ref, node_bias_ref, node_second_ref, node_gain_ref,
    out_ref, node_ref, *rest,
):
    slices, (table, total) = rest[:-2], rest[-2:]
    width = h_ref.shape[1]
    nodes = h_ref.shape[0]
    near = near_ref.shape[0]
    count = near + far_ref.shape[0]
    w_s = first_ref[0, width : 2 * width, :]
    table[0:near, :] = (dot(near_ref[...], w_s) * 0.5).astype(jnp.bfloat16)
    table[near:count, :] = (dot(far_ref[...], w_s) * 0.5).astype(jnp.bfloat16)
    received = dot(h_ref[0:COARSE, :], first_ref[0, 2 * width :, :]) + bias_ref[layer : layer + 1, :]
    table[count : count + COARSE, :] = (received * 0.5).astype(jnp.bfloat16)
    table[count + COARSE :, :] = jnp.zeros((128 - COARSE, width), jnp.bfloat16)
    w_edge = (first_ref[0, 0:width, :] * 0.5).astype(jnp.bfloat16)
    w_second = centred_columns(second_ref[0])
    gain_row = gain_ref[layer : layer + 1, :]
    heads = agg_ref[0:COARSE, :]
    for start in range(0, e_ref.shape[0], sub):
        rows = slice(start, start + sub)
        rcv = rcv_ref[:, rows]
        ends = jnp.concatenate(
            [onehot_lanes(column_of(idx_ref[:, rows]), count), onehot_lanes(column_of(rcv), 128)], axis=1
        )
        updated, message = edge_rows(e_ref[rows, :], ends, table[...], w_edge, w_second, gain_row)
        out_ref[rows, :] = updated
        heads += dot(onehot_sublanes(rcv, COARSE), message)
    total[0:COARSE, :] = heads.astype(jnp.bfloat16)
    total[COARSE:, :] = agg_ref[COARSE:, :].astype(jnp.bfloat16)
    h = h_ref[...]
    pre = (
        dot(h, node_first_ref[0, 0:width, :])
        + dot(total[...], node_first_ref[0, width:, :])
        + node_bias_ref[layer : layer + 1, :]
    )
    hidden = half_silu(pre * 0.5).astype(jnp.bfloat16)
    change = scale_rows(dot(hidden, centred_columns(node_second_ref[0])), node_gain_ref[layer : layer + 1, :])
    updated = (h.astype(jnp.float32) + change).astype(jnp.bfloat16)
    node_ref[...] = updated
    if slices:
        head, low, high = slices
        head[...] = updated[0:COARSE, :]
        low[...] = updated[0:HALO, :]
        high[...] = updated[nodes - HALO :, :]


def coarse_call(
    layer, e, idx, rcv, near, far, h, agg, first, bias, second, gain,
    node_first, node_bias, node_second, node_gain, sub, more,
):
    edges, width = e.shape
    nodes = h.shape[0]
    table_rows = near.shape[0] + far.shape[0] + 128
    whole = lambda i: (0, 0)
    this_layer = lambda i: (layer, 0, 0)
    full = lambda a: pl.BlockSpec(a.shape, whole)
    per_layer = lambda a: pl.BlockSpec((1,) + a.shape[1:], this_layer)
    idx = idx.reshape(1, edges)
    rcv = rcv.reshape(1, edges)
    outs = [(edges, width), (nodes, width)]
    if more:
        outs += [(COARSE, width), (HALO, width), (HALO, width)]
    return pl.pallas_call(
        functools.partial(coarse_kernel, layer, sub),
        grid=(1,),
        in_specs=[full(a) for a in (e, idx, rcv, near, far, h, agg)]
        + [per_layer(first), full(bias), per_layer(second), full(gain)]
        + [per_layer(node_first), full(node_bias), per_layer(node_second), full(node_gain)],
        out_specs=[pl.BlockSpec(s, whole) for s in outs],
        out_shape=[jax.ShapeDtypeStruct(s, jnp.bfloat16) for s in outs],
        scratch_shapes=[
            pltpu.VMEM((table_rows, width), jnp.bfloat16),
            pltpu.VMEM((nodes, width), jnp.bfloat16),
        ],
        cost_estimate=pl.CostEstimate(
            flops=2 * edges * width * (3 * width + table_rows) + 6 * nodes * width * width,
            bytes_accessed=8 << 20,
            transcendentals=0,
        ),
        name=f"coarse_{layer}",
    )(e, idx, rcv, near, far, h, agg, first, bias, second, gain, node_first, node_bias, node_second, node_gain)


def swap(value, axis, bit):
    count = lax.axis_size(axis)
    return lax.ppermute(value, axis, [(i, i ^ bit) for i in range(count)])


def turn(value, axis, by):
    count = lax.axis_size(axis)
    return lax.ppermute(value, axis, [(i, (i + by) % count) for i in range(count)])


def exchange(head, low, high):
    groups = lax.axis_size("group")
    patches = lax.axis_size("patch")
    below = turn(high, "patch", 1)
    above = turn(low, "patch", -1)
    line = jnp.concatenate([head] + [swap(head, "group", k) for k in range(1, groups)], axis=0)
    near = jnp.concatenate([line] + [swap(line, "patch", k) for k in range(2, patches, 2)], axis=0)
    far = swap(near, "patch", 1)
    return below, above, near, far


def body(
    node_latent, fine_latent, coarse_latent, fine_sender, fine_receiver, coarse_owner, coarse_row, coarse_receiver,
    edge_first, edge_bias, edge_second, edge_gain, node_first, node_bias, node_second, node_gain,
):
    groups = lax.axis_size("group")
    patches = lax.axis_size("patch")
    layers = edge_first.shape[0]
    owner = coarse_owner[:, 0]
    group_offset = (owner // patches) ^ lax.axis_index("group")
    patch_offset = (owner % patches) ^ lax.axis_index("patch")
    slot = ((patch_offset % 2) * (patches // 2) + patch_offset // 2) * groups + group_offset
    coarse_index = slot * COARSE + coarse_row
    h, fine, coarse = node_latent, fine_latent, coarse_latent
    head, low, high = h[:COARSE], h[:HALO], h[h.shape[0] - HALO :]
    for layer in range(layers):
        below, above, near, far = exchange(head, low, high)
        edge_weights = (edge_first, edge_bias, edge_second, edge_gain)
        fine, agg = fine_call(
            layer, fine, fine_sender, fine_receiver, h, below, above, *edge_weights, block=512, sub=256
        )
        last = layer == layers - 1
        out = coarse_call(
            layer, coarse, coarse_index, coarse_receiver, near, far, h, agg, *edge_weights,
            node_first, node_bias, node_second, node_gain, sub=256, more=not last,
        )
        coarse, h = out[:2]
        if not last:
            head, low, high = out[2:]
    return h, fine, coarse


def solution(mesh):
    rows = P(GP, None)
    flat = P(GP)
    in_specs = (rows, rows, rows, flat, flat, rows, flat, flat) + (P(),) * 8
    return jax.shard_map(body, mesh=mesh, in_specs=in_specs, out_specs=(rows, rows, rows), check_vma=False)
```

```python
import functools

import jax
import jax.numpy as jnp
from jax import lax
from jax.experimental import pallas as pl
from jax.experimental.pallas import tpu as pltpu
from jax.sharding import PartitionSpec as P


HALO = 64
COARSE = 16
EPSILON = 1e-05
GP = ("group", "patch")
LIMIT = 20 << 20


def dot(a, b):
    return jnp.dot(a, b, preferred_element_type=jnp.float32)


def half_silu(half):
    return half * jnp.tanh(half) + half


def centred_columns(weight):
    wide = weight.astype(jnp.float32)
    return (wide - jnp.mean(wide, axis=-1, keepdims=True)).astype(jnp.bfloat16)


def scale_rows(centred, gain_row):
    variance = jnp.mean(centred * centred, axis=-1, keepdims=True)
    return centred * lax.rsqrt(variance + EPSILON) * gain_row


def column_of(row):
    return jnp.transpose(jnp.broadcast_to(row, (128, row.shape[1])))


def onehot_lanes(column, count):
    lanes = lax.broadcasted_iota(jnp.int32, column.shape, 1)
    parts = [
        jnp.where(column == lanes + start, 1.0, 0.0).astype(jnp.bfloat16)
        for start in range(0, count, 128)
    ]
    return jnp.concatenate(parts, axis=1)


def onehot_sublanes(row, count):
    places = lax.broadcasted_iota(jnp.int32, (count, row.shape[1]), 0)
    return jnp.where(places == row, 1.0, 0.0).astype(jnp.bfloat16)


def edge_rows(latent, ends, table, weight_edge, weight_second, gain_row):
    half = dot(latent, weight_edge) + dot(ends, table)
    hidden = half_silu(half).astype(jnp.bfloat16)
    message = scale_rows(dot(hidden, weight_second), gain_row)
    updated = (latent.astype(jnp.float32) + message).astype(jnp.bfloat16)
    return updated, message.astype(jnp.bfloat16)


def fine_kernel(
    layer, sub, e_ref, snd_ref, rcv_ref, h_ref, lo_ref, hi_ref, first_ref, bias_ref, second_ref, gain_ref,
    out_ref, agg_ref, table, w_edge, w_second,
):
    nodes, width = h_ref.shape
    senders = nodes + 2 * HALO
    steps, _, block = snd_ref.shape
    w_s = first_ref[layer, width : 2 * width, :]
    h = h_ref[...]
    table[0:HALO, :] = (dot(lo_ref[...], w_s) * 0.5).astype(jnp.bfloat16)
    table[HALO : HALO + nodes, :] = (dot(h, w_s) * 0.5).astype(jnp.bfloat16)
    table[HALO + nodes : senders, :] = (dot(hi_ref[...], w_s) * 0.5).astype(jnp.bfloat16)
    received = dot(h, first_ref[layer, 2 * width :, :]) + bias_ref[layer : layer + 1, :]
    table[senders:, :] = (received * 0.5).astype(jnp.bfloat16)
    w_edge[...] = (first_ref[layer, 0:width, :] * 0.5).astype(jnp.bfloat16)
    w_second[...] = centred_columns(second_ref[layer])
    agg_ref[...] = jnp.zeros_like(agg_ref)
    gain_row = gain_ref[layer : layer + 1, :]

    @pl.loop(0, steps)
    def _(step):
        total = agg_ref[...]
        base = pl.multiple_of(step * block, block)
        for start in range(0, block, sub):
            snd = snd_ref[step, :, start : start + sub]
            rcv = rcv_ref[step, :, start : start + sub]
            from_sender = column_of(snd)
            from_receiver = column_of(rcv) + senders
            lanes = lax.broadcasted_iota(jnp.int32, from_sender.shape, 1)
            parts = []
            for place in range(0, senders + nodes, 128):
                hit = None
                if place < senders:
                    hit = from_sender == lanes + place
                if place + 128 > senders:
                    other = from_receiver == lanes + place
                    hit = other if hit is None else hit | other
                parts.append(jnp.where(hit, 1.0, 0.0).astype(jnp.bfloat16))
            ends = jnp.concatenate(parts, axis=1)
            rows = pl.ds(base + start, sub)
            updated, message = edge_rows(e_ref[rows, :], ends, table[...], w_edge[...], w_second[...], gain_row)
            out_ref[rows, :] = updated
            total += dot(onehot_sublanes(rcv, nodes), message)
        agg_ref[...] = total


VMEM = pl.BlockSpec(memory_space=pltpu.VMEM)


def fine_call(layer, e, snd, rcv, h, lo, hi, first, bias, second, gain, block, sub):
    edges, width = e.shape
    nodes = h.shape[0]
    steps = edges // block
    table_rows = 2 * nodes + 2 * HALO
    return pl.pallas_call(
        functools.partial(fine_kernel, layer, sub),
        in_specs=[VMEM] * 10,
        out_specs=[VMEM] * 2,
        out_shape=[
            jax.ShapeDtypeStruct((edges, width), jnp.bfloat16),
            jax.ShapeDtypeStruct((nodes, width), jnp.float32),
        ],
        scratch_shapes=[
            pltpu.VMEM((table_rows, width), jnp.bfloat16),
            pltpu.VMEM((width, width), jnp.bfloat16),
            pltpu.VMEM((width, width), jnp.bfloat16),
        ],
        compiler_params=pltpu.CompilerParams(vmem_limit_bytes=LIMIT),
        cost_estimate=pl.CostEstimate(
            flops=2 * edges * width * (2 * width + 2 * table_rows), bytes_accessed=8 << 20, transcendentals=0
        ),
    )(e, snd.reshape(steps, 1, block), rcv.reshape(steps, 1, block), h, lo, hi, first, bias, second, gain)


def coarse_kernel(
    layer, sub, e_ref, own_ref, row_ref, rcv_ref, near_ref, far_ref, h_ref, agg_ref,
    first_ref, bias_ref, second_ref, gain_ref,
    node_first_ref, node_bias_ref, node_second_ref, node_gain_ref,
    out_ref, node_ref, *rest,
):
    slices, (table, total) = rest[:-2], rest[-2:]
    nodes, width = h_ref.shape
    near = near_ref.shape[0]
    count = near + far_ref.shape[0]
    w_s = first_ref[layer, width : 2 * width, :]
    table[0:near, :] = (dot(near_ref[...], w_s) * 0.5).astype(jnp.bfloat16)
    table[near:count, :] = (dot(far_ref[...], w_s) * 0.5).astype(jnp.bfloat16)
    received = dot(h_ref[0:COARSE, :], first_ref[layer, 2 * width :, :]) + bias_ref[layer : layer + 1, :]
    table[count : count + COARSE, :] = (received * 0.5).astype(jnp.bfloat16)
    table[count + COARSE :, :] = jnp.zeros((128 - COARSE, width), jnp.bfloat16)
    w_edge = (first_ref[layer, 0:width, :] * 0.5).astype(jnp.bfloat16)
    w_second = centred_columns(second_ref[layer])
    gain_row = gain_ref[layer : layer + 1, :]
    groups = lax.axis_size("group")
    patches = lax.axis_size("patch")
    my_group = lax.axis_index("group")
    my_patch = lax.axis_index("patch")
    heads = agg_ref[0:COARSE, :]
    for start in range(0, e_ref.shape[0], sub):
        rows = slice(start, start + sub)
        rcv = rcv_ref[:, rows]
        owner = own_ref[:, rows]
        patch_offset = (owner & (patches - 1)) ^ my_patch
        group_offset = (owner >> (patches.bit_length() - 1)) ^ my_group
        slot = ((patch_offset & 1) * (patches // 2) + (patch_offset >> 1)) * groups + group_offset
        place = slot * COARSE + row_ref[:, rows]
        ends = jnp.concatenate(
            [onehot_lanes(column_of(place), count), onehot_lanes(column_of(rcv), 128)], axis=1
        )
        updated, message = edge_rows(e_ref[rows, :], ends, table[...], w_edge, w_second, gain_row)
        out_ref[rows, :] = updated
        heads += dot(onehot_sublanes(rcv, COARSE), message)
    total[0:COARSE, :] = heads.astype(jnp.bfloat16)
    total[COARSE:, :] = agg_ref[COARSE:, :].astype(jnp.bfloat16)
    h = h_ref[...]
    pre = (
        dot(h, node_first_ref[layer, 0:width, :])
        + dot(total[...], node_first_ref[layer, width:, :])
        + node_bias_ref[layer : layer + 1, :]
    )
    hidden = half_silu(pre * 0.5).astype(jnp.bfloat16)
    change = scale_rows(dot(hidden, centred_columns(node_second_ref[layer])), node_gain_ref[layer : layer + 1, :])
    updated = (h.astype(jnp.float32) + change).astype(jnp.bfloat16)
    node_ref[...] = updated
    if slices:
        head, low, high = slices
        head[...] = updated[0:COARSE, :]
        low[...] = updated[0:HALO, :]
        high[...] = updated[nodes - HALO :, :]


def coarse_call(
    layer, e, owner, row, rcv, near, far, h, agg, first, bias, second, gain,
    node_first, node_bias, node_second, node_gain, sub, more,
):
    edges, width = e.shape
    nodes = h.shape[0]
    table_rows = near.shape[0] + far.shape[0] + 128
    flat = lambda a: a.reshape(1, edges)
    outs = [(edges, width), (nodes, width)]
    if more:
        outs += [(COARSE, width), (HALO, width), (HALO, width)]
    return pl.pallas_call(
        functools.partial(coarse_kernel, layer, sub),
        in_specs=[VMEM] * 16,
        out_specs=[VMEM] * len(outs),
        out_shape=[jax.ShapeDtypeStruct(s, jnp.bfloat16) for s in outs],
        scratch_shapes=[
            pltpu.VMEM((table_rows, width), jnp.bfloat16),
            pltpu.VMEM((nodes, width), jnp.bfloat16),
        ],
        compiler_params=pltpu.CompilerParams(vmem_limit_bytes=LIMIT),
        cost_estimate=pl.CostEstimate(
            flops=2 * edges * width * (3 * width + table_rows) + 6 * nodes * width * width,
            bytes_accessed=8 << 20,
            transcendentals=0,
        ),
    )(
        e, flat(owner), flat(row), flat(rcv), near, far, h, agg, first, bias, second, gain,
        node_first, node_bias, node_second, node_gain,
    )


def open_kernel(h_ref, head_ref, low_ref, high_ref, sems):
    nodes = h_ref.shape[0]
    copies = [
        pltpu.make_async_copy(h_ref.at[0:COARSE, :], head_ref, sems.at[0]),
        pltpu.make_async_copy(h_ref.at[0:HALO, :], low_ref, sems.at[1]),
        pltpu.make_async_copy(h_ref.at[nodes - HALO : nodes, :], high_ref, sems.at[2]),
    ]
    for copy in copies:
        copy.start()
    for copy in copies:
        copy.wait()


def open_call(h):
    width = h.shape[1]
    outs = [(COARSE, width), (HALO, width), (HALO, width)]
    return pl.pallas_call(
        open_kernel,
        in_specs=[pl.BlockSpec(memory_space=pl.ANY)],
        out_specs=[VMEM] * 3,
        out_shape=[jax.ShapeDtypeStruct(s, jnp.bfloat16) for s in outs],
        scratch_shapes=[pltpu.SemaphoreType.DMA((3,))],
        compiler_params=pltpu.CompilerParams(vmem_limit_bytes=1 << 20),
        cost_estimate=pl.CostEstimate(flops=10**10, bytes_accessed=1 << 20, transcendentals=0),
        name="open",
    )(h)


def swap(value, axis, bit):
    count = lax.axis_size(axis)
    return lax.ppermute(value, axis, [(i, i ^ bit) for i in range(count)])


def turn(value, axis, by):
    count = lax.axis_size(axis)
    return lax.ppermute(value, axis, [(i, (i + by) % count) for i in range(count)])


def exchange(head, low, high):
    groups = lax.axis_size("group")
    patches = lax.axis_size("patch")
    parts = [head] + [swap(head, "group", k) for k in range(1, groups)]
    below = turn(high, "patch", 1)
    above = turn(low, "patch", -1)
    line = jnp.concatenate(parts, axis=0)
    parts = [line] + [swap(line, "patch", k) for k in range(2, patches, 2)]
    near = jnp.concatenate(parts, axis=0)
    far = swap(near, "patch", 1)
    return below, above, near, far


def body(
    node_latent, fine_latent, coarse_latent, fine_sender, fine_receiver, coarse_owner, coarse_row, coarse_receiver,
    edge_first, edge_bias, edge_second, edge_gain, node_first, node_bias, node_second, node_gain,
):
    layers = edge_first.shape[0]
    h, fine, coarse = node_latent, fine_latent, coarse_latent
    head, low, high = open_call(h)
    edge_weights = (edge_first, edge_bias, edge_second, edge_gain)
    node_weights = (node_first, node_bias, node_second, node_gain)
    for layer in range(layers):
        below, above, near, far = exchange(head, low, high)
        fine, agg = fine_call(
            layer, fine, fine_sender, fine_receiver, h, below, above, *edge_weights, block=512, sub=256
        )
        last = layer == layers - 1
        out = coarse_call(
            layer, coarse, coarse_owner, coarse_row, coarse_receiver, near, far, h, agg,
            *edge_weights, *node_weights, sub=256, more=not last,
        )
        coarse, h = out[:2]
        if not last:
            head, low, high = out[2:]
    return h, fine, coarse


def solution(mesh):
    assert all(size & (size - 1) == 0 for size in mesh.shape.values())
    rows = P(GP, None)
    flat = P(GP)
    in_specs = (rows, rows, rows, flat, flat, rows, flat, flat) + (P(),) * 8
    return jax.shard_map(body, mesh=mesh, in_specs=in_specs, out_specs=(rows, rows, rows), check_vma=False)
```

```python
import functools

import jax
import jax.numpy as jnp
from jax import lax
from jax.experimental import pallas as pl
from jax.experimental.pallas import tpu as pltpu
from jax.sharding import PartitionSpec as P


HALO = 64
COARSE = 16
EPSILON = 1e-05
GP = ("group", "patch")
LIMIT = 20 << 20


def dot(a, b):
    return jnp.dot(a, b, preferred_element_type=jnp.float32)


def half_silu(half):
    return half * jnp.tanh(half) + half


def centred_columns(weight):
    wide = weight.astype(jnp.float32)
    return (wide - jnp.mean(wide, axis=-1, keepdims=True)).astype(jnp.bfloat16)


def scale_rows(centred, gain_row):
    variance = jnp.mean(centred * centred, axis=-1, keepdims=True)
    return centred * lax.rsqrt(variance + EPSILON) * gain_row


def column_of(row):
    return jnp.transpose(jnp.broadcast_to(row, (128, row.shape[1])))


def onehot_lanes(column, count):
    lanes = lax.broadcasted_iota(jnp.int32, column.shape, 1)
    parts = [
        jnp.where(column == lanes + start, 1.0, 0.0).astype(jnp.bfloat16)
        for start in range(0, count, 128)
    ]
    return jnp.concatenate(parts, axis=1)


def onehot_sublanes(row, count):
    places = lax.broadcasted_iota(jnp.int32, (count, row.shape[1]), 0)
    return jnp.where(places == row, 1.0, 0.0).astype(jnp.bfloat16)


def edge_rows(latent, ends, table, weight_edge, weight_second, gain_row):
    half = dot(latent, weight_edge) + dot(ends, table)
    hidden = half_silu(half).astype(jnp.bfloat16)
    message = scale_rows(dot(hidden, weight_second), gain_row)
    updated = (latent.astype(jnp.float32) + message).astype(jnp.bfloat16)
    return updated, message.astype(jnp.bfloat16)


def fine_kernel(
    layer, sub, e_ref, snd_ref, rcv_ref, h_ref, lo_ref, hi_ref, first_ref, bias_ref, second_ref, gain_ref,
    out_ref, agg_ref, table, w_edge, w_second,
):
    nodes, width = h_ref.shape
    senders = nodes + 2 * HALO
    steps, _, block = snd_ref.shape
    w_s = first_ref[layer, width : 2 * width, :]
    h = h_ref[...]
    table[0:HALO, :] = (dot(lo_ref[...], w_s) * 0.5).astype(jnp.bfloat16)
    table[HALO : HALO + nodes, :] = (dot(h, w_s) * 0.5).astype(jnp.bfloat16)
    table[HALO + nodes : senders, :] = (dot(hi_ref[...], w_s) * 0.5).astype(jnp.bfloat16)
    received = dot(h, first_ref[layer, 2 * width :, :]) + bias_ref[layer : layer + 1, :]
    table[senders:, :] = (received * 0.5).astype(jnp.bfloat16)
    w_edge[...] = (first_ref[layer, 0:width, :] * 0.5).astype(jnp.bfloat16)
    w_second[...] = centred_columns(second_ref[layer])
    agg_ref[...] = jnp.zeros_like(agg_ref)
    gain_row = gain_ref[layer : layer + 1, :]

    def run(step):
        total = agg_ref[...]
        base = step * block
        for start in range(0, block, sub):
            snd = snd_ref[step, :, start : start + sub]
            rcv = rcv_ref[step, :, start : start + sub]
            from_sender = column_of(snd)
            from_receiver = column_of(rcv) + senders
            lanes = lax.broadcasted_iota(jnp.int32, from_sender.shape, 1)
            parts = []
            for place in range(0, senders + nodes, 128):
                hit = None
                if place < senders:
                    hit = from_sender == lanes + place
                if place + 128 > senders:
                    other = from_receiver == lanes + place
                    hit = other if hit is None else hit | other
                parts.append(jnp.where(hit, 1.0, 0.0).astype(jnp.bfloat16))
            ends = jnp.concatenate(parts, axis=1)
            rows = pl.ds(base + start, sub)
            updated, message = edge_rows(e_ref[rows, :], ends, table[...], w_edge[...], w_second[...], gain_row)
            out_ref[rows, :] = updated
            total += dot(onehot_sublanes(rcv, nodes), message)
        agg_ref[...] = total

    for step in range(steps):
        run(step)


VMEM = pl.BlockSpec(memory_space=pltpu.VMEM)


def fine_call(layer, e, snd, rcv, h, lo, hi, first, bias, second, gain, block, sub):
    edges, width = e.shape
    nodes = h.shape[0]
    steps = edges // block
    table_rows = 2 * nodes + 2 * HALO
    return pl.pallas_call(
        functools.partial(fine_kernel, layer, sub),
        in_specs=[VMEM] * 10,
        out_specs=[VMEM] * 2,
        out_shape=[
            jax.ShapeDtypeStruct((edges, width), jnp.bfloat16),
            jax.ShapeDtypeStruct((nodes, width), jnp.float32),
        ],
        scratch_shapes=[
            pltpu.VMEM((table_rows, width), jnp.bfloat16),
            pltpu.VMEM((width, width), jnp.bfloat16),
            pltpu.VMEM((width, width), jnp.bfloat16),
        ],
        compiler_params=pltpu.CompilerParams(vmem_limit_bytes=LIMIT),
        cost_estimate=pl.CostEstimate(
            flops=2 * edges * width * (2 * width + 2 * table_rows), bytes_accessed=8 << 20, transcendentals=0
        ),
    )(e, snd.reshape(steps, 1, block), rcv.reshape(steps, 1, block), h, lo, hi, first, bias, second, gain)


def near_kernel(
    layer, e_ref, own_ref, row_ref, rcv_ref, near_ref, h_ref, first_ref, bias_ref, second_ref,
    node_first_ref, node_bias_ref, node_second_ref,
    pre_ref, far_hot_ref, head_hot_ref, second_out, node_pre_ref, node_second_out, table,
):
    _, width = h_ref.shape
    near = near_ref.shape[0]
    groups = lax.axis_size("group")
    patches = lax.axis_size("patch")
    table[0:near, :] = (dot(near_ref[...], first_ref[layer, width : 2 * width, :]) * 0.5).astype(jnp.bfloat16)
    received = dot(h_ref[0:COARSE, :], first_ref[layer, 2 * width :, :]) + bias_ref[layer : layer + 1, :]
    table[near : near + COARSE, :] = (received * 0.5).astype(jnp.bfloat16)
    table[near + COARSE :, :] = jnp.zeros((128 - COARSE, width), jnp.bfloat16)
    w_edge = (first_ref[layer, 0:width, :] * 0.5).astype(jnp.bfloat16)
    owner = own_ref[...]
    rcv = rcv_ref[...]
    patch_offset = (owner & (patches - 1)) ^ lax.axis_index("patch")
    group_offset = (owner >> (patches.bit_length() - 1)) ^ lax.axis_index("group")
    slot = ((patch_offset & 1) * (patches // 2) + (patch_offset >> 1)) * groups + group_offset
    place = column_of(slot * COARSE + row_ref[...])
    ends = jnp.concatenate([onehot_lanes(place, near), onehot_lanes(column_of(rcv), 128)], axis=1)
    pre_ref[...] = dot(e_ref[...], w_edge) + dot(ends, table[...])
    far_hot_ref[...] = onehot_lanes(place - near, near)
    head_hot_ref[...] = onehot_sublanes(rcv, COARSE)
    second_out[...] = centred_columns(second_ref[layer])
    node_pre = dot(h_ref[...], node_first_ref[layer, 0:width, :]) + node_bias_ref[layer : layer + 1, :]
    node_pre_ref[...] = node_pre
    node_second_out[...] = centred_columns(node_second_ref[layer])


def near_call(
    layer, e, owner, row, rcv, near, h, first, bias, second, node_first, node_bias, node_second,
):
    edges, width = e.shape
    nodes = h.shape[0]
    count = near.shape[0]
    flat = lambda a: a.reshape(1, edges)
    outs = [
        ((edges, width), jnp.float32),
        ((edges, count), jnp.bfloat16),
        ((COARSE, edges), jnp.bfloat16),
        ((width, width), jnp.bfloat16),
        ((nodes, width), jnp.float32),
        ((width, width), jnp.bfloat16),
    ]
    return pl.pallas_call(
        functools.partial(near_kernel, layer),
        in_specs=[VMEM] * 12,
        out_specs=[VMEM] * len(outs),
        out_shape=[jax.ShapeDtypeStruct(*o) for o in outs],
        scratch_shapes=[pltpu.VMEM((count + 128, width), jnp.bfloat16)],
        compiler_params=pltpu.CompilerParams(vmem_limit_bytes=LIMIT),
        cost_estimate=pl.CostEstimate(
            flops=2 * edges * width * (width + count + 128), bytes_accessed=4 << 20, transcendentals=0
        ),
    )(
        e, flat(owner), flat(row), flat(rcv), near, h, first, bias, second, node_first, node_bias, node_second,
    )


def far_kernel(
    layer, last, e_ref, pre_ref, far_hot_ref, head_hot_ref, w_second, node_pre_ref, node_second, far_ref, h_ref,
    agg_ref, fine_ref, first_ref, gain_ref, node_first_ref, node_gain_ref, *rest,
):
    nodes, width = h_ref.shape
    if last:
        out_hbm, node_ref, fine_hbm, out_ref, sems = rest
        fine_copy = pltpu.make_async_copy(fine_ref, fine_hbm, sems.at[0])
        fine_copy.start()
    else:
        out_ref, node_ref, head_ref, low_ref, high_ref = rest
    table = (dot(far_ref[...], first_ref[layer, width : 2 * width, :]) * 0.5).astype(jnp.bfloat16)
    half = pre_ref[...] + dot(far_hot_ref[...], table)
    hidden = half_silu(half).astype(jnp.bfloat16)
    message = scale_rows(dot(hidden, w_second[...]), gain_ref[layer : layer + 1, :])
    out_ref[...] = (e_ref[...].astype(jnp.float32) + message).astype(jnp.bfloat16)
    if last:
        out_copy = pltpu.make_async_copy(out_ref, out_hbm, sems.at[1])
        out_copy.start()
    heads = agg_ref[0:COARSE, :] + dot(head_hot_ref[...], message.astype(jnp.bfloat16))
    w_total = node_first_ref[layer, width:, :]
    node_gain = node_gain_ref[layer : layer + 1, :]
    for start, stop, total in ((COARSE, nodes, agg_ref[COARSE:, :]), (0, COARSE, heads)):
        pre = node_pre_ref[start:stop, :] + dot(total.astype(jnp.bfloat16), w_total)
        node_hidden = half_silu(pre * 0.5).astype(jnp.bfloat16)
        change = scale_rows(dot(node_hidden, node_second[...]), node_gain)
        updated = (h_ref[start:stop, :].astype(jnp.float32) + change).astype(jnp.bfloat16)
        node_ref[start:stop, :] = updated
        if not last:
            if start == 0:
                head_ref[...] = updated
                low_ref[0:COARSE, :] = updated
            else:
                low_ref[COARSE:, :] = updated[0 : HALO - COARSE, :]
                high_ref[...] = updated[nodes - HALO - COARSE :, :]
    if last:
        fine_copy.wait()
        out_copy.wait()


def far_call(layer, last, e, partial, far, h, agg, fine, first, gain, node_first, node_gain):
    edges, width = e.shape
    nodes = h.shape[0]
    outs = [(edges, width), (nodes, width)]
    if last:
        outs += [fine.shape]
        hbm = pl.BlockSpec(memory_space=pl.ANY)
        out_specs = [hbm, VMEM, hbm]
        scratch = [pltpu.VMEM((edges, width), jnp.bfloat16), pltpu.SemaphoreType.DMA((2,))]
    else:
        outs += [(COARSE, width), (HALO, width), (HALO, width)]
        out_specs = [VMEM] * len(outs)
        scratch = []
    args = (e, *partial, far, h, agg, fine, first, gain, node_first, node_gain)
    return pl.pallas_call(
        functools.partial(far_kernel, layer, last),
        in_specs=[VMEM] * len(args),
        out_specs=out_specs,
        out_shape=[jax.ShapeDtypeStruct(s, jnp.bfloat16) for s in outs],
        scratch_shapes=scratch,
        compiler_params=pltpu.CompilerParams(vmem_limit_bytes=LIMIT),
        cost_estimate=pl.CostEstimate(
            flops=2 * edges * width * (2 * width + 2 * far.shape[0]) + 4 * nodes * width * width,
            bytes_accessed=4 << 20,
            transcendentals=0,
        ),
    )(*args)


def open_kernel(h_ref, head_ref, low_ref, high_ref, sems):
    nodes = h_ref.shape[0]
    copies = [
        pltpu.make_async_copy(h_ref.at[0:COARSE, :], head_ref, sems.at[0]),
        pltpu.make_async_copy(h_ref.at[0:HALO, :], low_ref, sems.at[1]),
        pltpu.make_async_copy(h_ref.at[nodes - HALO : nodes, :], high_ref, sems.at[2]),
    ]
    for copy in copies:
        copy.start()
    for copy in copies:
        copy.wait()


def open_call(h):
    width = h.shape[1]
    outs = [(COARSE, width), (HALO, width), (HALO, width)]
    return pl.pallas_call(
        open_kernel,
        in_specs=[pl.BlockSpec(memory_space=pl.ANY)],
        out_specs=[VMEM] * 3,
        out_shape=[jax.ShapeDtypeStruct(s, jnp.bfloat16) for s in outs],
        scratch_shapes=[pltpu.SemaphoreType.DMA((3,))],
        compiler_params=pltpu.CompilerParams(vmem_limit_bytes=1 << 20),
        cost_estimate=pl.CostEstimate(flops=10**10, bytes_accessed=1 << 20, transcendentals=0),
        name="open",
    )(h)


def swap(value, axis, bit):
    count = lax.axis_size(axis)
    return lax.ppermute(value, axis, [(i, i ^ bit) for i in range(count)])


def turn(value, axis, by):
    count = lax.axis_size(axis)
    return lax.ppermute(value, axis, [(i, (i + by) % count) for i in range(count)])


def exchange(head, low, high):
    groups = lax.axis_size("group")
    patches = lax.axis_size("patch")
    parts = [head] + [swap(head, "group", k) for k in range(1, groups)]
    below = turn(high, "patch", 1)
    above = turn(low, "patch", -1)
    line = jnp.concatenate(parts, axis=0)
    parts = [line] + [swap(line, "patch", k) for k in range(2, patches, 2)]
    near = jnp.concatenate(parts, axis=0)
    far = swap(near, "patch", 1)
    return below, above, near, far


def body(
    node_latent, fine_latent, coarse_latent, fine_sender, fine_receiver, coarse_owner, coarse_row, coarse_receiver,
    edge_first, edge_bias, edge_second, edge_gain, node_first, node_bias, node_second, node_gain,
):
    layers = edge_first.shape[0]
    h, fine, coarse = node_latent, fine_latent, coarse_latent
    head, low, high = open_call(h)
    edge_weights = (edge_first, edge_bias, edge_second, edge_gain)
    for layer in range(layers):
        below, above, near, far = exchange(head, low, high)
        fine, agg = fine_call(
            layer, fine, fine_sender, fine_receiver, h, below, above, *edge_weights, block=2048, sub=1024
        )
        last = layer == layers - 1
        partial = near_call(
            layer, coarse, coarse_owner, coarse_row, coarse_receiver, near, h,
            edge_first, edge_bias, edge_second, node_first, node_bias, node_second,
        )
        out = far_call(layer, last, coarse, partial, far, h, agg, fine, edge_first, edge_gain, node_first, node_gain)
        coarse, h = out[:2]
        if last:
            fine = out[2]
        else:
            head, low, high = out[2:]
    return h, fine, coarse


def solution(mesh):
    assert all(size & (size - 1) == 0 for size in mesh.shape.values())
    rows = P(GP, None)
    flat = P(GP)
    in_specs = (rows, rows, rows, flat, flat, rows, flat, flat) + (P(),) * 8
    return jax.shard_map(body, mesh=mesh, in_specs=in_specs, out_specs=(rows, rows, rows), check_vma=False)
```

```python
import functools

import jax
import jax.numpy as jnp
from jax import lax
from jax.experimental import pallas as pl
from jax.experimental.pallas import tpu as pltpu
from jax.sharding import PartitionSpec as P


HALO = 64
COARSE = 16
EPSILON = 1e-05
GP = ("group", "patch")
LIMIT = 20 << 20


def dot(a, b):
    return jnp.dot(a, b, preferred_element_type=jnp.float32)


def half_silu(half):
    return half * jnp.tanh(half) + half


def centred_columns(weight):
    wide = weight.astype(jnp.float32)
    return (wide - jnp.mean(wide, axis=-1, keepdims=True)).astype(jnp.bfloat16)


def scale_rows(centred, gain_row):
    variance = jnp.mean(centred * centred, axis=-1, keepdims=True)
    return centred * lax.rsqrt(variance + EPSILON) * gain_row


def column_of(row):
    return jnp.transpose(jnp.broadcast_to(row, (128, row.shape[1])))


def onehot_lanes(columns, start, count):
    lanes = lax.broadcasted_iota(jnp.int32, columns[0][2].shape, 1)
    parts = []
    for place in range(start, start + count, 128):
        hit = None
        for low, high, column in columns:
            if low < place + 128 and high > place:
                one = column == lanes + place
                hit = one if hit is None else hit | one
        parts.append(jnp.where(hit, 1.0, 0.0).astype(jnp.bfloat16))
    return jnp.concatenate(parts, axis=1)


def onehot_sublanes(row, count):
    places = lax.broadcasted_iota(jnp.int32, (count, row.shape[1]), 0)
    return jnp.where(places == row, 1.0, 0.0).astype(jnp.bfloat16)


def finish_rows(latent, half, weight_second, gain_row):
    hidden = half_silu(half).astype(jnp.bfloat16)
    message = scale_rows(dot(hidden, weight_second), gain_row)
    updated = (latent.astype(jnp.float32) + message).astype(jnp.bfloat16)
    return updated, message.astype(jnp.bfloat16)


def end_columns(snd, rcv, nodes):
    inner = HALO + nodes
    odd = lax.axis_index("patch") & 1
    before = 2 * nodes + odd * HALO
    after = 2 * nodes + (1 - odd) * HALO
    sender = jnp.where(snd < HALO, snd + before, jnp.where(snd < inner, snd - HALO, snd - inner + after))
    return column_of(sender), column_of(rcv + nodes)


def halves(value):
    return (value * 0.5).astype(jnp.bfloat16)


def prep_kernel(layer, h_ref, first_ref, bias_ref, second_ref, table_ref, tail_ref, w_edge, w_second):
    nodes, width = h_ref.shape
    split = table_ref.shape[0]
    h = h_ref[...]
    table_ref[0:nodes, :] = halves(dot(h, first_ref[layer, width : 2 * width, :]))
    received = halves(dot(h, first_ref[layer, 2 * width :, :]) + bias_ref[layer : layer + 1, :])
    table_ref[nodes:, :] = received[0 : split - nodes, :]
    tail_ref[...] = received[split - nodes :, :]
    w_edge[...] = halves(first_ref[layer, 0:width, :])
    w_second[...] = centred_columns(second_ref[layer])


VMEM = pl.BlockSpec(memory_space=pltpu.VMEM)


def call(kernel, args, outs, flops, scratch=(), out_specs=None, in_specs=None, limit=LIMIT):
    return pl.pallas_call(
        kernel,
        in_specs=in_specs or [VMEM] * len(args),
        out_specs=out_specs or [VMEM] * len(outs),
        out_shape=[jax.ShapeDtypeStruct(*o) for o in outs],
        scratch_shapes=list(scratch),
        compiler_params=pltpu.CompilerParams(vmem_limit_bytes=limit),
        cost_estimate=pl.CostEstimate(flops=flops, bytes_accessed=4 << 20, transcendentals=0),
    )(*args)


def prep_call(layer, h, first, bias, second):
    nodes, width = h.shape
    split = 2 * nodes // 256 * 256
    outs = [((rows, width), jnp.bfloat16) for rows in (split, 2 * nodes - split, width, width)]
    return call(functools.partial(prep_kernel, layer), (h, first, bias, second), outs, 4 * nodes * width * width)


def fine_kernel(
    layer, pieces, e_ref, snd_ref, rcv_ref, gain_ref, first_ref, w_edge, w_second, table_ref, tail_ref, sibling_ref,
    cross_ref, out_ref, agg_ref, last_table,
):
    width = e_ref.shape[1]
    nodes = agg_ref.shape[0]
    split = table_ref.shape[0]
    tail = tail_ref.shape[0]
    places = 2 * nodes + 2 * HALO
    w_s = first_ref[layer, width : 2 * width, :]
    last_table[0:tail, :] = tail_ref[...]
    last_table[tail : tail + HALO, :] = halves(dot(cross_ref[...], w_s))
    last_table[tail + HALO :, :] = halves(dot(sibling_ref[...], w_s))
    gain_row = gain_ref[layer : layer + 1, :]
    total = None
    for rows in pieces:
        rcv = rcv_ref[:, rows]
        sender, receiver = end_columns(snd_ref[:, rows], rcv, nodes)
        columns = [(0, nodes, sender), (nodes, 2 * nodes, receiver), (2 * nodes, places, sender)]
        half = (
            dot(e_ref[rows, :], w_edge[...])
            + dot(onehot_lanes(columns, 0, split), table_ref[...])
            + dot(onehot_lanes(columns, split, places - split), last_table[...])
        )
        updated, message = finish_rows(e_ref[rows, :], half, w_second[...], gain_row)
        out_ref[rows, :] = updated
        part = dot(onehot_sublanes(rcv, nodes), message)
        total = part if total is None else total + part
    agg_ref[...] = total


def fine_call(layer, pieces, e, snd, rcv, gain, first, prep, beside, across, nodes):
    edges, width = e.shape
    table, tail, w_edge, w_second = prep
    rows = tail.shape[0] + 2 * HALO
    return call(
        functools.partial(fine_kernel, layer, pieces),
        (e, snd, rcv, gain, first, w_edge, w_second, table, tail, beside, across),
        [((edges, width), jnp.bfloat16), ((nodes, width), jnp.float32)],
        2 * width * edges * (2 * width + table.shape[0] + rows + nodes),
        [pltpu.VMEM((rows, width), jnp.bfloat16)],
    )


def near_kernel(
    layer, e_ref, own_ref, row_ref, rcv_ref, near_ref, h_ref, agg_ref, w_edge, first_ref, bias_ref, node_first_ref,
    node_bias_ref, node_second_ref, node_gain_ref,
    pre_ref, far_hot_ref, head_hot_ref, head_pre_ref, node_second_out, others_ref, table,
):
    width = h_ref.shape[1]
    near = near_ref.shape[0]
    groups = lax.axis_size("group")
    patches = lax.axis_size("patch")
    table[0:near, :] = halves(dot(near_ref[...], first_ref[layer, width : 2 * width, :]))
    received = dot(h_ref[0:COARSE, :], first_ref[layer, 2 * width :, :]) + bias_ref[layer : layer + 1, :]
    table[near : near + COARSE, :] = halves(received)
    table[near + COARSE :, :] = jnp.zeros((128 - COARSE, width), jnp.bfloat16)
    owner = own_ref[...]
    rcv = rcv_ref[...]
    offset = (owner & (patches - 1)) ^ lax.axis_index("patch")
    group_offset = (owner >> (patches.bit_length() - 1)) ^ lax.axis_index("group")
    slot = ((offset & 1) * (patches // 2) + (offset >> 1)) * groups + group_offset
    place = column_of(slot * COARSE + row_ref[...])
    ends = onehot_lanes([(0, near, place), (near, near + 128, column_of(rcv + near))], 0, near + 128)
    pre_ref[...] = dot(e_ref[...], w_edge[...]) + dot(ends, table[...])
    far_hot_ref[...] = onehot_lanes([(near, 2 * near, place)], near, near)
    head_hot_ref[...] = onehot_sublanes(rcv, COARSE)
    node_pre = dot(h_ref[...], node_first_ref[layer, 0:width, :]) + node_bias_ref[layer : layer + 1, :]
    head_pre_ref[...] = node_pre[0:COARSE, :]
    node_second_out[...] = centred_columns(node_second_ref[layer])
    others_ref[...] = update_nodes(
        h_ref[COARSE:, :], node_pre[COARSE:, :], agg_ref[COARSE:, :], node_first_ref[layer, width:, :],
        node_second_out[...], node_gain_ref[layer : layer + 1, :],
    )


def update_nodes(h, node_pre, total, w_total, w_second, gain_row):
    pre = node_pre + dot(total.astype(jnp.bfloat16), w_total)
    hidden = half_silu(pre * 0.5).astype(jnp.bfloat16)
    change = scale_rows(dot(hidden, w_second), gain_row)
    return (h.astype(jnp.float32) + change).astype(jnp.bfloat16)


def near_call(
    layer, e, owner, row, rcv, near, h, agg, w_edge, first, bias, node_first, node_bias, node_second, node_gain
):
    edges, width = e.shape
    nodes = h.shape[0]
    count = near.shape[0]
    flat = lambda a: a.reshape(1, edges)
    outs = [
        ((edges, width), jnp.float32),
        ((edges, count), jnp.bfloat16),
        ((COARSE, edges), jnp.bfloat16),
        ((COARSE, width), jnp.float32),
        ((width, width), jnp.bfloat16),
        ((nodes - COARSE, width), jnp.bfloat16),
    ]
    args = (
        e, flat(owner), flat(row), flat(rcv), near, h, agg, w_edge, first, bias,
        node_first, node_bias, node_second, node_gain,
    )
    return call(
        functools.partial(near_kernel, layer), args, outs,
        2 * width * (edges * (width + count + 128) + 3 * nodes * width),
        [pltpu.VMEM((count + 128, width), jnp.bfloat16)],
    )


def far_kernel(
    layer, last, e_ref, pre_ref, far_hot_ref, head_hot_ref, head_pre_ref, node_second, others_ref, w_second, far_ref,
    h_ref, agg_ref, fine_ref, first_ref, gain_ref, node_first_ref, node_gain_ref, *rest,
):
    nodes, width = h_ref.shape
    copies = []

    def send(source, target):
        copies.append(pltpu.make_async_copy(source, target, sems.at[len(copies)]))
        copies[-1].start()

    if last:
        out_hbm, node_hbm, fine_hbm, out_ref, head_ref, sems = rest
        send(fine_ref, fine_hbm)
        send(others_ref, node_hbm.at[COARSE:nodes, :])
    else:
        out_ref, node_ref, head_ref, cross_ref, sibling_ref = rest
    table = halves(dot(far_ref[...], first_ref[layer, width : 2 * width, :]))
    half = pre_ref[...] + dot(far_hot_ref[...], table)
    updated, message = finish_rows(e_ref[...], half, w_second[...], gain_ref[layer : layer + 1, :])
    out_ref[...] = updated
    if last:
        send(out_ref, out_hbm)
    heads = agg_ref[0:COARSE, :] + dot(head_hot_ref[...], message)
    head = update_nodes(
        h_ref[0:COARSE, :], head_pre_ref[...], heads, node_first_ref[layer, width:, :], node_second[...],
        node_gain_ref[layer : layer + 1, :],
    )
    head_ref[...] = head
    if last:
        send(head_ref, node_hbm.at[0:COARSE, :])
        for copy in copies:
            copy.wait()
    else:
        others = others_ref[...]
        node_ref[0:COARSE, :] = head
        node_ref[COARSE:, :] = others
        low = jnp.concatenate([head, others[0 : HALO - COARSE, :]], axis=0)
        high = others[nodes - HALO - COARSE :, :]
        odd = (lax.axis_index("patch") & 1) == 1
        cross_ref[...] = jnp.where(odd, high, low)
        sibling_ref[...] = jnp.where(odd, low, high)


def far_call(layer, last, e, partial, w_second, far, h, agg, fine, first, gain, node_first, node_gain):
    edges, width = e.shape
    nodes = h.shape[0]
    outs = [(edges, width), (nodes, width)]
    if last:
        outs += [fine.shape]
        out_specs = [pl.BlockSpec(memory_space=pl.ANY)] * 3
        scratch = [pltpu.VMEM((n, width), jnp.bfloat16) for n in (edges, COARSE)] + [pltpu.SemaphoreType.DMA((4,))]
    else:
        outs += [(COARSE, width), (HALO, width), (HALO, width)]
        out_specs = None
        scratch = []
    args = (e, *partial, w_second, far, h, agg, fine, first, gain, node_first, node_gain)
    return call(
        functools.partial(far_kernel, layer, last), args, [(o, jnp.bfloat16) for o in outs],
        2 * width * (edges * (width + far.shape[0]) + far.shape[0] * width + 2 * nodes * width),
        scratch, out_specs,
    )


def open_kernel(h_ref, head_ref, cross_ref, sibling_ref, sems):
    nodes = h_ref.shape[0]
    odd = lax.axis_index("patch") & 1
    upper = pl.multiple_of(odd * (nodes - HALO), HALO)
    lower = pl.multiple_of((1 - odd) * (nodes - HALO), HALO)
    copies = [
        pltpu.make_async_copy(h_ref.at[0:COARSE, :], head_ref, sems.at[0]),
        pltpu.make_async_copy(h_ref.at[pl.ds(upper, HALO), :], cross_ref, sems.at[1]),
        pltpu.make_async_copy(h_ref.at[pl.ds(lower, HALO), :], sibling_ref, sems.at[2]),
    ]
    for copy in copies:
        copy.start()
    for copy in copies:
        copy.wait()


def open_call(h):
    width = h.shape[1]
    outs = [((n, width), jnp.bfloat16) for n in (COARSE, HALO, HALO)]
    return call(
        open_kernel, (h,), outs, 10**10, [pltpu.SemaphoreType.DMA((3,))],
        in_specs=[pl.BlockSpec(memory_space=pl.ANY)], limit=1 << 20,
    )


def swap(value, axis, bit):
    count = lax.axis_size(axis)
    return lax.ppermute(value, axis, [(i, i ^ bit) for i in range(count)])


def exchange(head, cross, sibling):
    groups = lax.axis_size("group")
    patches = lax.axis_size("patch")
    parts = [head] + [swap(head, "group", k) for k in range(1, groups)]
    beside = swap(sibling, "patch", 1)
    pairs = [(p, (p + (1 if p % 2 else -1)) % patches) for p in range(patches)]
    across = lax.ppermute(cross, "patch", pairs)
    line = jnp.concatenate(parts, axis=0)
    parts = [line] + [swap(line, "patch", k) for k in range(2, patches, 2)]
    near = jnp.concatenate(parts, axis=0)
    far = swap(near, "patch", 1)
    return beside, across, near, far


def body(
    node_latent, fine_latent, coarse_latent, fine_sender, fine_receiver, coarse_owner, coarse_row, coarse_receiver,
    edge_first, edge_bias, edge_second, edge_gain, node_first, node_bias, node_second, node_gain,
):
    layers = edge_first.shape[0]
    h, fine, coarse = node_latent, fine_latent, coarse_latent
    edges = fine.shape[0]
    nodes = h.shape[0]
    snd = fine_sender.reshape(1, edges)
    rcv = fine_receiver.reshape(1, edges)
    pieces = [slice(0, edges // 2), slice(edges // 2, edges)]
    head, cross, sibling = open_call(h)
    for layer in range(layers):
        last = layer == layers - 1
        beside, across, near, far = exchange(head, cross, sibling)
        prep = prep_call(layer, h, edge_first, edge_bias, edge_second)
        fine, agg = fine_call(
            layer, pieces, fine, snd, rcv, edge_gain, edge_first, prep, beside, across, nodes
        )
        partial = near_call(
            layer, coarse, coarse_owner, coarse_row, coarse_receiver, near, h, agg, prep[2],
            edge_first, edge_bias, node_first, node_bias, node_second, node_gain,
        )
        out = far_call(
            layer, last, coarse, partial, prep[3], far, h, agg, fine,
            edge_first, edge_gain, node_first, node_gain,
        )
        coarse, h = out[:2]
        if last:
            fine = out[2]
        else:
            head, cross, sibling = out[2:]
    return h, fine, coarse


def solution(mesh):
    assert all(size & (size - 1) == 0 for size in mesh.shape.values())
    rows = P(GP, None)
    flat = P(GP)
    in_specs = (rows, rows, rows, flat, flat, rows, flat, flat) + (P(),) * 8
    return jax.shard_map(body, mesh=mesh, in_specs=in_specs, out_specs=(rows, rows, rows), check_vma=False)
```

```python
import functools

import jax
import jax.numpy as jnp
from jax import lax
from jax.experimental import pallas as pl
from jax.experimental.pallas import tpu as pltpu
from jax.sharding import PartitionSpec as P


HALO = 64
COARSE = 16
EPSILON = 1e-05
GP = ("group", "patch")
LIMIT = 20 << 20


def dot(a, b):
    return jnp.dot(a, b, preferred_element_type=jnp.float32)


def half_silu(half):
    return half * jnp.tanh(half) + half


def centred_columns(weight):
    wide = weight.astype(jnp.float32)
    return (wide - jnp.mean(wide, axis=-1, keepdims=True)).astype(jnp.bfloat16)


def scale_rows(centred, gain_row):
    variance = jnp.mean(centred * centred, axis=-1, keepdims=True)
    return centred * lax.rsqrt(variance + EPSILON) * gain_row


def column_of(row):
    return jnp.transpose(jnp.broadcast_to(row, (128, row.shape[1])))


def onehot_lanes(columns, start, count):
    lanes = lax.broadcasted_iota(jnp.int32, columns[0][2].shape, 1)
    parts = []
    for place in range(start, start + count, 128):
        hit = None
        for low, high, column in columns:
            if low < place + 128 and high > place:
                one = column == lanes + place
                hit = one if hit is None else hit | one
        parts.append(jnp.where(hit, 1.0, 0.0).astype(jnp.bfloat16))
    return jnp.concatenate(parts, axis=1)


def onehot_sublanes(row, count):
    places = lax.broadcasted_iota(jnp.int32, (count, row.shape[1]), 0)
    return jnp.where(places == row, 1.0, 0.0).astype(jnp.bfloat16)


def finish_rows(latent, half, weight_second, gain_row):
    hidden = half_silu(half).astype(jnp.bfloat16)
    message = scale_rows(dot(hidden, weight_second), gain_row)
    updated = (latent.astype(jnp.float32) + message).astype(jnp.bfloat16)
    return updated, message.astype(jnp.bfloat16)


def end_columns(snd, rcv, nodes):
    inner = HALO + nodes
    odd = lax.axis_index("patch") & 1
    before = 2 * nodes + odd * HALO
    after = 2 * nodes + (1 - odd) * HALO
    sender = jnp.where(snd < HALO, snd + before, jnp.where(snd < inner, snd - HALO, snd - inner + after))
    return column_of(sender), column_of(rcv + nodes)


def halves(value):
    return (value * 0.5).astype(jnp.bfloat16)


def prep_kernel(layer, h_ref, first_ref, bias_ref, second_ref, table_ref, tail_ref, w_edge, w_second):
    nodes, width = h_ref.shape
    split = table_ref.shape[0]
    h = h_ref[...]
    table_ref[0:nodes, :] = halves(dot(h, first_ref[layer, width : 2 * width, :]))
    received = halves(dot(h, first_ref[layer, 2 * width :, :]) + bias_ref[layer : layer + 1, :])
    table_ref[nodes:, :] = received[0 : split - nodes, :]
    tail_ref[...] = received[split - nodes :, :]
    w_edge[...] = halves(first_ref[layer, 0:width, :])
    w_second[...] = centred_columns(second_ref[layer])


VMEM = pl.BlockSpec(memory_space=pltpu.VMEM)


def call(kernel, args, outs, flops, scratch=(), out_specs=None, in_specs=None, limit=LIMIT):
    return pl.pallas_call(
        kernel,
        in_specs=in_specs or [VMEM] * len(args),
        out_specs=out_specs or [VMEM] * len(outs),
        out_shape=[jax.ShapeDtypeStruct(*o) for o in outs],
        scratch_shapes=list(scratch),
        compiler_params=pltpu.CompilerParams(vmem_limit_bytes=limit),
        cost_estimate=pl.CostEstimate(flops=flops, bytes_accessed=4 << 20, transcendentals=0),
    )(*args)


def prep_call(layer, h, first, bias, second):
    nodes, width = h.shape
    split = 2 * nodes // 256 * 256
    outs = [((rows, width), jnp.bfloat16) for rows in (split, 2 * nodes - split, width, width)]
    return call(functools.partial(prep_kernel, layer), (h, first, bias, second), outs, 4 * nodes * width * width)


def fine_kernel(
    layer, pieces, e_ref, snd_ref, rcv_ref, gain_ref, first_ref, w_edge, w_second, table_ref, tail_ref, sibling_ref,
    cross_ref, out_ref, agg_ref, last_table,
):
    width = e_ref.shape[1]
    nodes = agg_ref.shape[0]
    split = table_ref.shape[0]
    tail = tail_ref.shape[0]
    places = 2 * nodes + 2 * HALO
    w_s = first_ref[layer, width : 2 * width, :]
    last_table[0:tail, :] = tail_ref[...]
    last_table[tail : tail + HALO, :] = halves(dot(cross_ref[...], w_s))
    last_table[tail + HALO :, :] = halves(dot(sibling_ref[...], w_s))
    gain_row = gain_ref[layer : layer + 1, :]
    total = None
    for rows in pieces:
        rcv = rcv_ref[:, rows]
        sender, receiver = end_columns(snd_ref[:, rows], rcv, nodes)
        columns = [(0, nodes, sender), (nodes, 2 * nodes, receiver), (2 * nodes, places, sender)]
        half = (
            dot(e_ref[rows, :], w_edge[...])
            + dot(onehot_lanes(columns, 0, split), table_ref[...])
            + dot(onehot_lanes(columns, split, places - split), last_table[...])
        )
        updated, message = finish_rows(e_ref[rows, :], half, w_second[...], gain_row)
        out_ref[rows, :] = updated
        part = dot(onehot_sublanes(rcv, nodes), message)
        total = part if total is None else total + part
    agg_ref[...] = total


def fine_call(layer, pieces, e, snd, rcv, gain, first, prep, beside, across, nodes):
    edges, width = e.shape
    table, tail, w_edge, w_second = prep
    rows = tail.shape[0] + 2 * HALO
    return call(
        functools.partial(fine_kernel, layer, pieces),
        (e, snd, rcv, gain, first, w_edge, w_second, table, tail, beside, across),
        [((edges, width), jnp.bfloat16), ((nodes, width), jnp.float32)],
        2 * width * edges * (2 * width + table.shape[0] + rows + nodes),
        [pltpu.VMEM((rows, width), jnp.bfloat16)],
    )


def near_kernel(
    layer, e_ref, own_ref, row_ref, rcv_ref, near_ref, h_ref, agg_ref, w_edge, first_ref, bias_ref, node_first_ref,
    node_bias_ref, node_second_ref, node_gain_ref,
    pre_ref, far_hot_ref, head_hot_ref, head_pre_ref, node_second_out, others_ref, table,
):
    width = h_ref.shape[1]
    near = near_ref.shape[0]
    groups = lax.axis_size("group")
    patches = lax.axis_size("patch")
    table[0:near, :] = halves(dot(near_ref[...], first_ref[layer, width : 2 * width, :]))
    received = dot(h_ref[0:COARSE, :], first_ref[layer, 2 * width :, :]) + bias_ref[layer : layer + 1, :]
    table[near : near + COARSE, :] = halves(received)
    table[near + COARSE :, :] = jnp.zeros((128 - COARSE, width), jnp.bfloat16)
    owner = own_ref[...]
    rcv = rcv_ref[...]
    offset = (owner & (patches - 1)) ^ lax.axis_index("patch")
    group_offset = (owner >> (patches.bit_length() - 1)) ^ lax.axis_index("group")
    slot = ((offset & 1) * (patches // 2) + (offset >> 1)) * groups + group_offset
    place = column_of(slot * COARSE + row_ref[...])
    ends = onehot_lanes([(0, near, place), (near, near + 128, column_of(rcv + near))], 0, near + 128)
    pre_ref[...] = dot(e_ref[...], w_edge[...]) + dot(ends, table[...])
    far_hot_ref[...] = onehot_lanes([(near, 2 * near, place)], near, near)
    head_hot_ref[...] = onehot_sublanes(rcv, COARSE)
    node_pre = dot(h_ref[...], node_first_ref[layer, 0:width, :]) + node_bias_ref[layer : layer + 1, :]
    head_pre_ref[...] = node_pre[0:COARSE, :]
    node_second_out[...] = centred_columns(node_second_ref[layer])
    others_ref[...] = update_nodes(
        h_ref[COARSE:, :], node_pre[COARSE:, :], agg_ref[COARSE:, :], node_first_ref[layer, width:, :],
        node_second_out[...], node_gain_ref[layer : layer + 1, :],
    )


def update_nodes(h, node_pre, total, w_total, w_second, gain_row):
    pre = node_pre + dot(total.astype(jnp.bfloat16), w_total)
    hidden = half_silu(pre * 0.5).astype(jnp.bfloat16)
    change = scale_rows(dot(hidden, w_second), gain_row)
    return (h.astype(jnp.float32) + change).astype(jnp.bfloat16)


def near_call(
    layer, e, owner, row, rcv, near, h, agg, w_edge, first, bias, node_first, node_bias, node_second, node_gain
):
    edges, width = e.shape
    nodes = h.shape[0]
    count = near.shape[0]
    flat = lambda a: a.reshape(1, edges)
    outs = [
        ((edges, width), jnp.float32),
        ((edges, count), jnp.bfloat16),
        ((COARSE, edges), jnp.bfloat16),
        ((COARSE, width), jnp.float32),
        ((width, width), jnp.bfloat16),
        ((nodes - COARSE, width), jnp.bfloat16),
    ]
    args = (
        e, flat(owner), flat(row), flat(rcv), near, h, agg, w_edge, first, bias,
        node_first, node_bias, node_second, node_gain,
    )
    return call(
        functools.partial(near_kernel, layer), args, outs,
        2 * width * (edges * (width + count + 128) + 3 * nodes * width),
        [pltpu.VMEM((count + 128, width), jnp.bfloat16)],
    )


def far_kernel(
    layer, last, e_ref, pre_ref, far_hot_ref, head_hot_ref, head_pre_ref, node_second, others_ref, w_second, far_ref,
    h_ref, agg_ref, fine_ref, first_ref, gain_ref, node_first_ref, node_gain_ref, *rest,
):
    nodes, width = h_ref.shape
    copies = []

    def send(source, target):
        copies.append(pltpu.make_async_copy(source, target, sems.at[len(copies)]))
        copies[-1].start()

    if last:
        out_hbm, node_hbm, fine_hbm, out_ref, head_ref, sems = rest
        send(fine_ref, fine_hbm)
        send(others_ref, node_hbm.at[COARSE:nodes, :])
    else:
        out_ref, node_ref, head_ref, cross_ref, sibling_ref = rest
    table = halves(dot(far_ref[...], first_ref[layer, width : 2 * width, :]))
    half = pre_ref[...] + dot(far_hot_ref[...], table)
    updated, message = finish_rows(e_ref[...], half, w_second[...], gain_ref[layer : layer + 1, :])
    out_ref[...] = updated
    if last:
        send(out_ref, out_hbm)
    heads = agg_ref[0:COARSE, :] + dot(head_hot_ref[...], message)
    head = update_nodes(
        h_ref[0:COARSE, :], head_pre_ref[...], heads, node_first_ref[layer, width:, :], node_second[...],
        node_gain_ref[layer : layer + 1, :],
    )
    head_ref[...] = head
    if last:
        send(head_ref, node_hbm.at[0:COARSE, :])
        for copy in copies:
            copy.wait()
    else:
        others = others_ref[...]
        node_ref[0:COARSE, :] = head
        node_ref[COARSE:, :] = others
        low = jnp.concatenate([head, others[0 : HALO - COARSE, :]], axis=0)
        high = others[nodes - HALO - COARSE :, :]
        odd = (lax.axis_index("patch") & 1) == 1
        cross_ref[...] = jnp.where(odd, high, low)
        sibling_ref[...] = jnp.where(odd, low, high)


def far_call(layer, last, e, partial, w_second, far, h, agg, fine, first, gain, node_first, node_gain):
    edges, width = e.shape
    nodes = h.shape[0]
    outs = [(edges, width), (nodes, width)]
    if last:
        outs += [fine.shape]
        out_specs = [pl.BlockSpec(memory_space=pl.ANY)] * 3
        scratch = [pltpu.VMEM((n, width), jnp.bfloat16) for n in (edges, COARSE)] + [pltpu.SemaphoreType.DMA((4,))]
    else:
        outs += [(COARSE, width), (HALO, width), (HALO, width)]
        out_specs = None
        scratch = []
    args = (e, *partial, w_second, far, h, agg, fine, first, gain, node_first, node_gain)
    return call(
        functools.partial(far_kernel, layer, last), args, [(o, jnp.bfloat16) for o in outs],
        2 * width * (edges * (width + far.shape[0]) + far.shape[0] * width + 2 * nodes * width),
        scratch, out_specs,
    )


def open_kernel(h_ref, head_ref, cross_ref, sibling_ref, sems):
    nodes = h_ref.shape[0]
    odd = lax.axis_index("patch") & 1
    upper = pl.multiple_of(odd * (nodes - HALO), HALO)
    lower = pl.multiple_of((1 - odd) * (nodes - HALO), HALO)
    copies = [
        pltpu.make_async_copy(h_ref.at[0:COARSE, :], head_ref, sems.at[0]),
        pltpu.make_async_copy(h_ref.at[pl.ds(upper, HALO), :], cross_ref, sems.at[1]),
        pltpu.make_async_copy(h_ref.at[pl.ds(lower, HALO), :], sibling_ref, sems.at[2]),
    ]
    for copy in copies:
        copy.start()
    for copy in copies:
        copy.wait()


def open_call(h):
    width = h.shape[1]
    outs = [((n, width), jnp.bfloat16) for n in (COARSE, HALO, HALO)]
    return call(
        open_kernel, (h,), outs, 10**10, [pltpu.SemaphoreType.DMA((3,))],
        in_specs=[pl.BlockSpec(memory_space=pl.ANY)], limit=1 << 20,
    )


def swap(value, axis, bit):
    count = lax.axis_size(axis)
    return lax.ppermute(value, axis, [(i, i ^ bit) for i in range(count)])


def exchange(head, cross, sibling):
    groups = lax.axis_size("group")
    patches = lax.axis_size("patch")
    parts = [head]
    for k in range(1, groups):
        parts.append(swap(head, "group", k))
    beside = swap(sibling, "patch", 1)
    pairs = [(p, (p + (1 if p % 2 else -1)) % patches) for p in range(patches)]
    across = lax.ppermute(cross, "patch", pairs)
    line = jnp.concatenate(parts, axis=0)
    parts = [line]
    for k in range(2, patches, 2):
        parts.append(swap(line, "patch", k))
    near = jnp.concatenate(parts, axis=0)
    far = swap(near, "patch", 1)
    return beside, across, near, far


def body(
    node_latent, fine_latent, coarse_latent, fine_sender, fine_receiver, coarse_owner, coarse_row, coarse_receiver,
    edge_first, edge_bias, edge_second, edge_gain, node_first, node_bias, node_second, node_gain,
):
    layers = edge_first.shape[0]
    h, fine, coarse = node_latent, fine_latent, coarse_latent
    edges = fine.shape[0]
    nodes = h.shape[0]
    snd = fine_sender.reshape(1, edges)
    rcv = fine_receiver.reshape(1, edges)
    pieces = [slice(0, edges // 2), slice(edges // 2, edges)]
    head, cross, sibling = open_call(h)
    for layer in range(layers):
        last = layer == layers - 1
        beside, across, near, far = exchange(head, cross, sibling)
        prep = prep_call(layer, h, edge_first, edge_bias, edge_second)
        fine, agg = fine_call(
            layer, pieces, fine, snd, rcv, edge_gain, edge_first, prep, beside, across, nodes
        )
        partial = near_call(
            layer, coarse, coarse_owner, coarse_row, coarse_receiver, near, h, agg, prep[2],
            edge_first, edge_bias, node_first, node_bias, node_second, node_gain,
        )
        out = far_call(
            layer, last, coarse, partial, prep[3], far, h, agg, fine,
            edge_first, edge_gain, node_first, node_gain,
        )
        coarse, h = out[:2]
        if last:
            fine = out[2]
        else:
            head, cross, sibling = out[2:]
    return h, fine, coarse


def solution(mesh):
    assert all(size & (size - 1) == 0 for size in mesh.shape.values())
    rows = P(GP, None)
    flat = P(GP)
    in_specs = (rows, rows, rows, flat, flat, rows, flat, flat) + (P(),) * 8
    return jax.shard_map(body, mesh=mesh, in_specs=in_specs, out_specs=(rows, rows, rows), check_vma=False)
```

```python
import functools

import jax
import jax.numpy as jnp
from jax import lax
from jax.experimental import pallas as pl
from jax.experimental.pallas import tpu as pltpu
from jax.sharding import PartitionSpec as P


HALO = 64
COARSE = 16
EPSILON = 1e-05
GP = ("group", "patch")
LIMIT = 20 << 20


def dot(a, b):
    return jnp.dot(a, b, preferred_element_type=jnp.float32)


def half_silu(half):
    return half * jnp.tanh(half) + half


def centred_columns(weight):
    wide = weight.astype(jnp.float32)
    return (wide - jnp.mean(wide, axis=-1, keepdims=True)).astype(jnp.bfloat16)


def scale_rows(centred, gain_row):
    variance = jnp.mean(centred * centred, axis=-1, keepdims=True)
    return centred * lax.rsqrt(variance + EPSILON) * gain_row


def column_of(row):
    return jnp.transpose(jnp.broadcast_to(row, (128, row.shape[1])))


def onehot_lanes(columns, start, count):
    lanes = lax.broadcasted_iota(jnp.int32, columns[0][2].shape, 1)
    parts = []
    for place in range(start, start + count, 128):
        hit = None
        for low, high, column in columns:
            if low < place + 128 and high > place:
                one = column == lanes + place
                hit = one if hit is None else hit | one
        parts.append(jnp.where(hit, 1.0, 0.0).astype(jnp.bfloat16))
    return jnp.concatenate(parts, axis=1)


def onehot_sublanes(row, count):
    places = lax.broadcasted_iota(jnp.int32, (count, row.shape[1]), 0)
    return jnp.where(places == row, 1.0, 0.0).astype(jnp.bfloat16)


def finish_rows(latent, half, weight_second, gain_row):
    hidden = half_silu(half).astype(jnp.bfloat16)
    message = scale_rows(dot(hidden, weight_second), gain_row)
    updated = (latent.astype(jnp.float32) + message).astype(jnp.bfloat16)
    return updated, message.astype(jnp.bfloat16)


def end_columns(snd, rcv, nodes):
    inner = HALO + nodes
    odd = lax.axis_index("patch") & 1
    before = 2 * nodes + odd * HALO
    after = 2 * nodes + (1 - odd) * HALO
    sender = jnp.where(snd < HALO, snd + before, jnp.where(snd < inner, snd - HALO, snd - inner + after))
    return column_of(sender), column_of(rcv + nodes)


def halves(value):
    return (value * 0.5).astype(jnp.bfloat16)


def prep_kernel(layer, h_ref, first_ref, bias_ref, second_ref, table_ref, tail_ref, w_edge, w_second):
    nodes, width = h_ref.shape
    split = table_ref.shape[0]
    h = h_ref[...]
    table_ref[0:nodes, :] = halves(dot(h, first_ref[layer, width : 2 * width, :]))
    received = halves(dot(h, first_ref[layer, 2 * width :, :]) + bias_ref[layer : layer + 1, :])
    table_ref[nodes:, :] = received[0 : split - nodes, :]
    tail_ref[...] = received[split - nodes :, :]
    w_edge[...] = halves(first_ref[layer, 0:width, :])
    w_second[...] = centred_columns(second_ref[layer])


VMEM = pl.BlockSpec(memory_space=pltpu.VMEM)


def call(kernel, args, outs, flops, scratch=(), out_specs=None, in_specs=None, limit=LIMIT):
    return pl.pallas_call(
        kernel,
        in_specs=in_specs or [VMEM] * len(args),
        out_specs=out_specs or [VMEM] * len(outs),
        out_shape=[jax.ShapeDtypeStruct(*o) for o in outs],
        scratch_shapes=list(scratch),
        compiler_params=pltpu.CompilerParams(vmem_limit_bytes=limit),
        cost_estimate=pl.CostEstimate(flops=flops, bytes_accessed=4 << 20, transcendentals=0),
    )(*args)


def prep_call(layer, h, first, bias, second):
    nodes, width = h.shape
    split = 2 * nodes // 256 * 256
    outs = [((rows, width), jnp.bfloat16) for rows in (split, 2 * nodes - split, width, width)]
    return call(functools.partial(prep_kernel, layer), (h, first, bias, second), outs, 4 * nodes * width * width)


def fine_kernel(
    layer, pieces, e_ref, snd_ref, rcv_ref, gain_ref, first_ref, w_edge, w_second, table_ref, tail_ref, sibling_ref,
    cross_ref, out_ref, agg_ref, last_table,
):
    width = e_ref.shape[1]
    nodes = agg_ref.shape[0]
    split = table_ref.shape[0]
    tail = tail_ref.shape[0]
    places = 2 * nodes + 2 * HALO
    w_s = first_ref[layer, width : 2 * width, :]
    last_table[0:tail, :] = tail_ref[...]
    last_table[tail : tail + HALO, :] = halves(dot(cross_ref[...], w_s))
    last_table[tail + HALO :, :] = halves(dot(sibling_ref[...], w_s))
    gain_row = gain_ref[layer : layer + 1, :]
    total = None
    for rows in pieces:
        rcv = rcv_ref[:, rows]
        sender, receiver = end_columns(snd_ref[:, rows], rcv, nodes)
        columns = [(0, nodes, sender), (nodes, 2 * nodes, receiver), (2 * nodes, places, sender)]
        half = (
            dot(e_ref[rows, :], w_edge[...])
            + dot(onehot_lanes(columns, 0, split), table_ref[...])
            + dot(onehot_lanes(columns, split, places - split), last_table[...])
        )
        updated, message = finish_rows(e_ref[rows, :], half, w_second[...], gain_row)
        out_ref[rows, :] = updated
        part = dot(onehot_sublanes(rcv, nodes), message)
        total = part if total is None else total + part
    agg_ref[...] = total


def fine_call(layer, pieces, e, snd, rcv, gain, first, prep, beside, across, nodes):
    edges, width = e.shape
    table, tail, w_edge, w_second = prep
    rows = tail.shape[0] + 2 * HALO
    return call(
        functools.partial(fine_kernel, layer, pieces),
        (e, snd, rcv, gain, first, w_edge, w_second, table, tail, beside, across),
        [((edges, width), jnp.bfloat16), ((nodes, width), jnp.float32)],
        2 * width * edges * (2 * width + table.shape[0] + rows + nodes),
        [pltpu.VMEM((rows, width), jnp.bfloat16)],
    )


def near_kernel(
    layer, e_ref, own_ref, row_ref, rcv_ref, near_ref, h_ref, agg_ref, w_edge, first_ref, bias_ref, node_first_ref,
    node_bias_ref, node_second_ref, node_gain_ref,
    pre_ref, far_hot_ref, head_hot_ref, head_pre_ref, node_second_out, others_ref, table,
):
    width = h_ref.shape[1]
    near = near_ref.shape[0]
    groups = lax.axis_size("group")
    patches = lax.axis_size("patch")
    table[0:near, :] = halves(dot(near_ref[...], first_ref[layer, width : 2 * width, :]))
    received = dot(h_ref[0:COARSE, :], first_ref[layer, 2 * width :, :]) + bias_ref[layer : layer + 1, :]
    table[near : near + COARSE, :] = halves(received)
    table[near + COARSE :, :] = jnp.zeros((128 - COARSE, width), jnp.bfloat16)
    owner = own_ref[...]
    rcv = rcv_ref[...]
    offset = (owner & (patches - 1)) ^ lax.axis_index("patch")
    group_offset = (owner >> (patches.bit_length() - 1)) ^ lax.axis_index("group")
    offset = offset ^ jnp.where(group_offset != 0, 1, 0)
    far = (offset & 1) ^ jnp.where(offset >= 2, 1, 0)
    slot = (far * (patches // 2) + (offset >> 1)) * groups + group_offset
    place = column_of(slot * COARSE + row_ref[...])
    ends = onehot_lanes([(0, near, place), (near, near + 128, column_of(rcv + near))], 0, near + 128)
    pre_ref[...] = dot(e_ref[...], w_edge[...]) + dot(ends, table[...])
    far_hot_ref[...] = onehot_lanes([(near, 2 * near, place)], near, near)
    head_hot_ref[...] = onehot_sublanes(rcv, COARSE)
    node_pre = dot(h_ref[...], node_first_ref[layer, 0:width, :]) + node_bias_ref[layer : layer + 1, :]
    head_pre_ref[...] = node_pre[0:COARSE, :]
    node_second_out[...] = centred_columns(node_second_ref[layer])
    others_ref[...] = update_nodes(
        h_ref[COARSE:, :], node_pre[COARSE:, :], agg_ref[COARSE:, :], node_first_ref[layer, width:, :],
        node_second_out[...], node_gain_ref[layer : layer + 1, :],
    )


def update_nodes(h, node_pre, total, w_total, w_second, gain_row):
    pre = node_pre + dot(total.astype(jnp.bfloat16), w_total)
    hidden = half_silu(pre * 0.5).astype(jnp.bfloat16)
    change = scale_rows(dot(hidden, w_second), gain_row)
    return (h.astype(jnp.float32) + change).astype(jnp.bfloat16)


def near_call(
    layer, e, owner, row, rcv, near, h, agg, w_edge, first, bias, node_first, node_bias, node_second, node_gain
):
    edges, width = e.shape
    nodes = h.shape[0]
    count = near.shape[0]
    flat = lambda a: a.reshape(1, edges)
    outs = [
        ((edges, width), jnp.float32),
        ((edges, count), jnp.bfloat16),
        ((COARSE, edges), jnp.bfloat16),
        ((COARSE, width), jnp.float32),
        ((width, width), jnp.bfloat16),
        ((nodes - COARSE, width), jnp.bfloat16),
    ]
    args = (
        e, flat(owner), flat(row), flat(rcv), near, h, agg, w_edge, first, bias,
        node_first, node_bias, node_second, node_gain,
    )
    return call(
        functools.partial(near_kernel, layer), args, outs,
        2 * width * (edges * (width + count + 128) + 3 * nodes * width),
        [pltpu.VMEM((count + 128, width), jnp.bfloat16)],
    )


def far_kernel(
    layer, last, e_ref, pre_ref, far_hot_ref, head_hot_ref, head_pre_ref, node_second, others_ref, w_second, far_ref,
    h_ref, agg_ref, fine_ref, first_ref, gain_ref, node_first_ref, node_gain_ref, *rest,
):
    nodes, width = h_ref.shape
    copies = []

    def send(source, target):
        copies.append(pltpu.make_async_copy(source, target, sems.at[len(copies)]))
        copies[-1].start()

    if last:
        out_hbm, node_hbm, fine_hbm, out_ref, head_ref, sems = rest
        send(fine_ref, fine_hbm)
        send(others_ref, node_hbm.at[COARSE:nodes, :])
    else:
        out_ref, node_ref, head_ref, cross_ref, sibling_ref = rest
    table = halves(dot(far_ref[...], first_ref[layer, width : 2 * width, :]))
    half = pre_ref[...] + dot(far_hot_ref[...], table)
    updated, message = finish_rows(e_ref[...], half, w_second[...], gain_ref[layer : layer + 1, :])
    out_ref[...] = updated
    if last:
        send(out_ref, out_hbm)
    heads = agg_ref[0:COARSE, :] + dot(head_hot_ref[...], message)
    head = update_nodes(
        h_ref[0:COARSE, :], head_pre_ref[...], heads, node_first_ref[layer, width:, :], node_second[...],
        node_gain_ref[layer : layer + 1, :],
    )
    head_ref[...] = head
    if last:
        send(head_ref, node_hbm.at[0:COARSE, :])
        for copy in copies:
            copy.wait()
    else:
        others = others_ref[...]
        node_ref[0:COARSE, :] = head
        node_ref[COARSE:, :] = others
        low = jnp.concatenate([head, others[0 : HALO - COARSE, :]], axis=0)
        high = others[nodes - HALO - COARSE :, :]
        odd = (lax.axis_index("patch") & 1) == 1
        cross_ref[...] = jnp.where(odd, high, low)
        sibling_ref[...] = jnp.where(odd, low, high)


def far_call(layer, last, e, partial, w_second, far, h, agg, fine, first, gain, node_first, node_gain):
    edges, width = e.shape
    nodes = h.shape[0]
    outs = [(edges, width), (nodes, width)]
    if last:
        outs += [fine.shape]
        out_specs = [pl.BlockSpec(memory_space=pl.ANY)] * 3
        scratch = [pltpu.VMEM((n, width), jnp.bfloat16) for n in (edges, COARSE)] + [pltpu.SemaphoreType.DMA((4,))]
    else:
        outs += [(COARSE, width), (HALO, width), (HALO, width)]
        out_specs = None
        scratch = []
    args = (e, *partial, w_second, far, h, agg, fine, first, gain, node_first, node_gain)
    return call(
        functools.partial(far_kernel, layer, last), args, [(o, jnp.bfloat16) for o in outs],
        2 * width * (edges * (width + far.shape[0]) + far.shape[0] * width + 2 * nodes * width),
        scratch, out_specs,
    )


def open_kernel(h_ref, head_ref, cross_ref, sibling_ref, sems):
    nodes = h_ref.shape[0]
    odd = lax.axis_index("patch") & 1
    upper = pl.multiple_of(odd * (nodes - HALO), HALO)
    lower = pl.multiple_of((1 - odd) * (nodes - HALO), HALO)
    copies = [
        pltpu.make_async_copy(h_ref.at[0:COARSE, :], head_ref, sems.at[0]),
        pltpu.make_async_copy(h_ref.at[pl.ds(upper, HALO), :], cross_ref, sems.at[1]),
        pltpu.make_async_copy(h_ref.at[pl.ds(lower, HALO), :], sibling_ref, sems.at[2]),
    ]
    for copy in copies:
        copy.start()
    for copy in copies:
        copy.wait()


def open_call(h):
    width = h.shape[1]
    outs = [((n, width), jnp.bfloat16) for n in (COARSE, HALO, HALO)]
    return call(
        open_kernel, (h,), outs, 10**10, [pltpu.SemaphoreType.DMA((3,))],
        in_specs=[pl.BlockSpec(memory_space=pl.ANY)], limit=1 << 20,
    )


def swap(value, axis, bit):
    count = lax.axis_size(axis)
    return lax.ppermute(value, axis, [(i, i ^ bit) for i in range(count)])


def exchange(head, cross, sibling):
    groups = lax.axis_size("group")
    patches = lax.axis_size("patch")
    parts = [head]
    for k in range(1, groups):
        parts.append(swap(head, GP, k * patches + 1))
    beside = swap(sibling, "patch", 1)
    pairs = [(p, (p + (1 if p % 2 else -1)) % patches) for p in range(patches)]
    across = lax.ppermute(cross, "patch", pairs)
    line = jnp.concatenate(parts, axis=0)
    parts = [line]
    for k in range(3, patches, 2):
        parts.append(swap(line, "patch", k))
    near = jnp.concatenate(parts, axis=0)
    far = swap(near, "patch", 1)
    return beside, across, near, far


def body(
    node_latent, fine_latent, coarse_latent, fine_sender, fine_receiver, coarse_owner, coarse_row, coarse_receiver,
    edge_first, edge_bias, edge_second, edge_gain, node_first, node_bias, node_second, node_gain,
):
    layers = edge_first.shape[0]
    h, fine, coarse = node_latent, fine_latent, coarse_latent
    edges = fine.shape[0]
    nodes = h.shape[0]
    snd = fine_sender.reshape(1, edges)
    rcv = fine_receiver.reshape(1, edges)
    pieces = [slice(0, edges // 2), slice(edges // 2, edges)]
    head, cross, sibling = open_call(h)
    for layer in range(layers):
        last = layer == layers - 1
        beside, across, near, far = exchange(head, cross, sibling)
        prep = prep_call(layer, h, edge_first, edge_bias, edge_second)
        fine, agg = fine_call(
            layer, pieces, fine, snd, rcv, edge_gain, edge_first, prep, beside, across, nodes
        )
        partial = near_call(
            layer, coarse, coarse_owner, coarse_row, coarse_receiver, near, h, agg, prep[2],
            edge_first, edge_bias, node_first, node_bias, node_second, node_gain,
        )
        out = far_call(
            layer, last, coarse, partial, prep[3], far, h, agg, fine,
            edge_first, edge_gain, node_first, node_gain,
        )
        coarse, h = out[:2]
        if last:
            fine = out[2]
        else:
            head, cross, sibling = out[2:]
    return h, fine, coarse


def solution(mesh):
    assert all(size & (size - 1) == 0 for size in mesh.shape.values())
    rows = P(GP, None)
    flat = P(GP)
    in_specs = (rows, rows, rows, flat, flat, rows, flat, flat) + (P(),) * 8
    return jax.shard_map(body, mesh=mesh, in_specs=in_specs, out_specs=(rows, rows, rows), check_vma=False)
```
